256 devices in a mesh: ang: 32 (over y, z_lo, core), sl: 8 (over z_hi, x).
Axes of the slice: x: 4, y: 4, z: 8 (z_hi: 2, z_lo: 4; z = z_hi * 4 + z_lo), core: 2. Of those that a mesh axis runs over, the one named last changes fastest.
Arguments:
- sinogram: bfloat16 [64, 64, 1024], P('sl', 'ang'), may hold values from -72 to 72
- detector_coord: int32 [64, 64, 512], P('ang', 'sl'), may hold values from 0 to 1072693247
Outputs:
- image_rows: float32 [64, 64, 512], P('ang', 'sl')
The draws below stay inside these ranges and needn't reach their ends.
All inputs are finite; a program needn't handle non-finite values.
Results may differ from the reference program's by a relative error of at most 0.0052.
Values may be sent and summed in bfloat16 or wider, within the bound.
A program may use at most 64 MiB of HBM per device.

```python
import math
import jax
import jax.numpy as jnp
from jax import lax

BINS = 1024
IMG = 512
SLICES = 64
ANGLES = 64
ROWS = 64


def place_ends(result, own_key, least, high):
    index_at = [jax.random.randint(jax.random.fold_in(own_key, axis), (), 0, length) for axis, length in enumerate(result.shape)]
    longest = result.shape.index(max(result.shape))
    beside = index_at[:longest] + [(index_at[longest] + 1) % result.shape[longest]] + index_at[longest + 1:]
    return result.at[tuple(index_at)].set(least).at[tuple(beside)].set(high)


def levels(key, shape, split, low, high):
    gain, own = 1.0, jax.random.fold_in(key, 6)
    for dim, parts in split:
        heights = jnp.exp(jax.random.uniform(jax.random.fold_in(own, dim), (parts,), jnp.float32, low / len(split), high / len(split)))
        gain = gain * jnp.repeat(heights, shape[dim] // parts).reshape([-1 if axis == dim else 1 for axis in range(len(shape))])
    return gain


def bell_draw(rng, dims, scale, reach, shards=(), kind=jnp.bfloat16):
    values = scale * jax.random.normal(rng, dims, jnp.float32)
    if shards:
        values = values * levels(rng, dims, shards, -0.22, 0.18)
    return jnp.clip(values, -reach, reach).astype(kind)


def setup_inputs(seed: int = 0) -> dict:
    key_list = jax.random.split(jax.random.key(seed), 3)
    return {
        "sinogram": bell_draw(key_list[0], (SLICES, ANGLES, BINS), 12.0, 72.0, ((0, 8), (1, 32))),
        "detector_coord": place_ends(jax.random.randint(key_list[1], (ANGLES, ROWS, IMG), 0, (BINS - 1) * 1048576), jax.random.fold_in(key_list[1], 1), 0, ((BINS - 1) * 1048576) - 1).astype(jnp.int32),
    }


def ramp_table(bin_count):
    first = lax.broadcasted_iota(jnp.int32, (bin_count, bin_count), 0)
    second = lax.broadcasted_iota(jnp.int32, (bin_count, bin_count), 1)
    offset = second - first
    offset_sq = jnp.maximum((offset * offset).astype(jnp.float32), jnp.float32(1.0))
    odd_mask = (offset % 2) != 0
    values = jnp.where(offset == 0, jnp.float32(0.25), jnp.where(odd_mask, jnp.float32(-1.0 / (math.pi ** 2)) / offset_sq, jnp.float32(0.0)))
    return values.astype(jnp.bfloat16)


def interp_weights(row_coords, bin_count):
    bin_left = row_coords // 1048576
    fraction = (row_coords % 1048576).astype(jnp.float32) / jnp.float32(1048576.0)
    positions = lax.broadcasted_iota(jnp.int32, row_coords.shape + (bin_count,), 2)
    left_part = jnp.where(positions == bin_left[..., None], 1.0 - fraction[..., None], jnp.float32(0.0))
    right_part = jnp.where(positions == bin_left[..., None] + 1, fraction[..., None], jnp.float32(0.0))
    return (left_part + right_part).astype(jnp.bfloat16)


def reference(sinogram, detector_coord):
    slices, angles, bin_count = sinogram.shape
    table = ramp_table(bin_count)
    filtered = jnp.dot(sinogram.reshape(slices * angles, bin_count), table, preferred_element_type=jnp.float32)
    filtered = filtered.astype(jnp.bfloat16).reshape(slices, angles, bin_count)

    def add_angle(running, angle_step):
        projection = lax.dynamic_index_in_dim(filtered, angle_step, 1, keepdims=False)
        row_coords = lax.dynamic_index_in_dim(detector_coord, angle_step, 0, keepdims=False)
        weights = interp_weights(row_coords, bin_count)
        contrib = jnp.einsum('rxb,sb->rsx', weights.astype(jnp.float32), projection.astype(jnp.float32))
        return running + contrib, None

    start_value = jnp.zeros((detector_coord.shape[1], slices, detector_coord.shape[2]), jnp.float32)
    running, unused = lax.scan(add_angle, start_value, jnp.arange(angles, dtype=jnp.int32))
    return running * jnp.float32(math.pi / angles)
```

```python
import math

import jax
import jax.numpy as jnp
from jax import lax
from jax.experimental import pallas as pl
from jax.experimental.pallas import tpu as pltpu
from jax.sharding import PartitionSpec as P

MESH = pl.DeviceIdType.MESH
NY, NZ, NC, NH, NX = 4, 4, 2, 2, 4
NK = NY * NC


def flip(bit, by):
    return bit + by - 2 * bit * by


def lane_gather(table, lanes):
    return jnp.take_along_axis(table, lanes, axis=1, mode="promise_in_bounds")


def write_ramp(g_ref):
    depth, width = g_ref.shape

    def chunk(step, carry):
        base = pl.multiple_of(step * 16, 16)
        for lane in range(0, width, 256):
            row = lax.broadcasted_iota(jnp.int32, (16, 256), 0) + base
            column = lax.broadcasted_iota(jnp.int32, (16, 256), 1) + (lane - 768)
            offset = column - row
            real = offset.astype(jnp.float32)
            square = jnp.maximum(real * real, jnp.float32(1.0))
            odd = (offset & 1) != 0
            value = jnp.where(odd, jnp.float32(-1.0 / math.pi**2) / square, jnp.float32(0.0))
            value = jnp.where(offset == 0, jnp.float32(0.25), value)
            g_ref[pl.ds(base, 16), lane : lane + 256] = value.astype(jnp.bfloat16)
        return carry

    lax.fori_loop(0, depth // 16, chunk, 0)


def kernel(
    x_ref, c_ref, o_ref,
    csend, sbuf, cbuf, g_ref, f_ref, t_ref, sc_ref, obuf, rbuf,
    s_send, s_recv, c_send, c_recv, w_send, w_recv, o_send, o_recv,
):
    ang, sl = lax.axis_index("ang"), lax.axis_index("sl")
    y, z, c = ang // 8, (ang // 2) % 4, ang % 2
    h, x = sl // 4, sl % 4

    def device(yy, zz, cc, hh, xx):
        return (yy * 8 + zz * 2 + cc, hh * 4 + xx)

    def near(dy, dc, dh):
        return device((y + dy) % NY, z, flip(c, dc), flip(h, dh), x)

    along_x = [device(y, z, c, h, (x + dx) % NX) for dx in range(1, NX)]
    owners = []
    for dh in range(NH):
        for dx in range(NX):
            block = flip(h, dh) * NX + (x - dx) % NX
            owners.append((4 * block + y, sl))
    sources = [((ang % 4) * 8 + zz * 2 + cc, sl) for zz in range(NZ) for cc in range(NC)]

    barrier = pltpu.get_barrier_semaphore()
    group = [near(dy, dc, dh) for dh in range(NH) for dy in range(NY) for dc in range(NC)][1:]
    group += along_x + owners + sources
    for other in group:
        pl.semaphore_signal(barrier, inc=1, device_id=other, device_id_type=MESH)
    for a in range(2):
        for p in range(4):
            csend[:, a, p, :] = c_ref[a, :, 128 * p : 128 * (p + 1)]
    pl.semaphore_wait(barrier, len(group))

    first = {}
    for dh in (1, 0):
        for dy in range(NY):
            for dc in range(NC):
                k = dy * NC + dc
                row = 2 * ((y + dy) % NY) + flip(c, dc)
                if (dh, k) == (0, 0):
                    cbuf[0, :, 0, :, :] = csend[row]
                    continue
                copy = pltpu.make_async_remote_copy(
                    src_ref=csend.at[row],
                    dst_ref=cbuf.at[k, :, dh * NX],
                    send_sem=c_send.at[dh, k],
                    recv_sem=c_recv.at[dh, k],
                    device_id=near(dy, dc, dh),
                    device_id_type=MESH,
                )
                copy.start()
                first[dh, k] = copy
    sino = []
    for dy in range(NY):
        for dc in range(NC):
            k = dy * NC + dc
            if k == 0:
                sbuf[0] = x_ref[...]
                continue
            copy = pltpu.make_async_remote_copy(
                src_ref=x_ref,
                dst_ref=sbuf.at[k],
                send_sem=s_send.at[k],
                recv_sem=s_recv.at[k],
                device_id=near(dy, dc, 0),
                device_id_type=MESH,
            )
            copy.start()
            sino.append(copy)

    write_ramp(g_ref)

    def forward(dh):
        copies = []
        for k in range(NK):
            if (dh, k) in first:
                first[dh, k].wait_recv()
        for dx in range(1, NX):
            copy = pltpu.make_async_remote_copy(
                src_ref=cbuf.at[:, :, dh * NX],
                dst_ref=cbuf.at[:, :, dh * NX + dx],
                send_sem=w_send.at[dh, dx],
                recv_sem=w_recv.at[dh, dx],
                device_id=along_x[dx - 1],
                device_id_type=MESH,
            )
            copy.start()
            copies.append(copy)
        return copies

    passed = {0: forward(0), 1: forward(1)}

    for copy in sino:
        copy.wait_recv()
    lhs = sbuf[...].reshape(NK * 16, 1024)
    for n in range(4):
        total = None
        for m in range(4):
            at = 768 - 256 * m + 256 * n
            part = jnp.dot(
                lhs[:, 256 * m : 256 * (m + 1)], g_ref[:, at : at + 256],
                preferred_element_type=jnp.float32,
            )
            total = part if total is None else total + part
        f_ref[2 * n] = total[:, :128]
        f_ref[2 * n + 1] = total[:, 128:]

    def pack(k, carry):
        for a in range(2):
            rows = pl.ds(k * 16 + a, 8, stride=2)
            value = jnp.concatenate([f_ref[n, rows, :] for n in range(8)], axis=1)
            top = jnp.maximum(jnp.max(jnp.abs(value), axis=1, keepdims=True), jnp.float32(1e-30))
            fixed = (value * (jnp.float32(32767.0) / top) + jnp.float32(32768.5)).astype(jnp.int32)
            fixed = fixed - 32768
            after = pltpu.roll(fixed, 1023, 1)
            t_ref[k, a] = (fixed << 16) | (after & 0xFFFF)
            sc_ref[k, a] = jnp.broadcast_to(top * jnp.float32(1.0 / 32767.0), (8, 128))
        return carry

    lax.fori_loop(0, NK, pack, 0)

    own = z * NC + c
    sent = []
    for dh in range(NH):
        for copy in passed[dh]:
            copy.wait_recv()

        def source(k, sums, dh=dh):
            sums = list(sums)
            for a in range(2):
                table = [t_ref[k, a, :, 128 * n : 128 * (n + 1)] for n in range(8)]
                scale = sc_ref[k, a]
                for dx in range(NX):
                    for p in range(4):
                        coord = cbuf[k, a, dh * NX + dx, p : p + 1, :]
                        coord = jnp.broadcast_to(coord, (8, 128))
                        left = coord >> 20
                        fraction = (coord & 0xFFFFF).astype(jnp.float32)
                        fraction = fraction * jnp.float32(1.0 / 1048576.0)
                        lanes = left & 127
                        found = [lane_gather(part, lanes) for part in table]
                        for bit in (128, 256, 512):
                            on = (left & bit) != 0
                            found = [
                                jnp.where(on, found[i + 1], found[i])
                                for i in range(0, len(found), 2)
                            ]
                        word = found[0]
                        low = (word >> 16).astype(jnp.float32)
                        high = ((word << 16) >> 16).astype(jnp.float32)
                        value = low + (high - low) * fraction
                        at = dx * 4 + p
                        sums[at] = sums[at] + value * scale
            return tuple(sums)

        zero = jnp.zeros((8, 128), jnp.float32)
        sums = lax.fori_loop(0, NK, source, (zero,) * 16)
        for dx in range(NX):
            slot = dh * NX + dx
            for p in range(4):
                obuf[slot, :, 128 * p : 128 * (p + 1)] = sums[dx * 4 + p].astype(jnp.bfloat16)
            copy = pltpu.make_async_remote_copy(
                src_ref=obuf.at[slot],
                dst_ref=rbuf.at[own],
                send_sem=o_send.at[slot],
                recv_sem=o_recv.at[own],
                device_id=owners[slot],
                device_id_type=MESH,
            )
            mine = owners[slot][0] == ang

            @pl.when(jnp.logical_not(mine))
            def _():
                copy.start()

            @pl.when(mine)
            def _():
                rbuf[own] = obuf[slot]

            sent.append((copy, mine))

    for at, source_device in enumerate(sources):
        arrival = pltpu.make_async_remote_copy(
            src_ref=obuf.at[0],
            dst_ref=rbuf.at[at],
            send_sem=o_send.at[0],
            recv_sem=o_recv.at[at],
            device_id=source_device,
            device_id_type=MESH,
        )

        @pl.when(source_device[0] != ang)
        def _():
            arrival.wait_recv()

    for cc in range(NC):
        total = rbuf[cc].astype(jnp.float32)
        for zz in range(1, NZ):
            total = total + rbuf[zz * NC + cc].astype(jnp.float32)
        o_ref[cc] = total * jnp.float32(math.pi / 64)

    for copy, mine in sent:

        @pl.when(jnp.logical_not(mine))
        def _():
            copy.wait_send()

    for copy in [*first.values(), *sino, *passed[0], *passed[1]]:
        copy.wait_send()


def shards(sinogram, detector_coord):
    dma = pltpu.SemaphoreType.DMA
    vmem = pl.BlockSpec(memory_space=pltpu.VMEM)
    return pl.pallas_call(
        kernel,
        out_shape=jax.ShapeDtypeStruct((2, 8, 512), jnp.float32),
        in_specs=[vmem, vmem],
        out_specs=vmem,
        scratch_shapes=[
            pltpu.VMEM((8, 2, 4, 128), jnp.int32),
            pltpu.VMEM((NK, 8, 2, 1024), jnp.bfloat16),
            pltpu.VMEM((NK, 2, 8, 4, 128), jnp.int32),
            pltpu.VMEM((256, 1792), jnp.bfloat16),
            pltpu.VMEM((8, NK * 16, 128), jnp.float32),
            pltpu.VMEM((NK, 2, 8, 1024), jnp.int32),
            pltpu.VMEM((NK, 2, 8, 128), jnp.float32),
            pltpu.VMEM((8, 8, 512), jnp.bfloat16),
            pltpu.VMEM((8, 8, 512), jnp.bfloat16),
            dma((NK,)), dma((NK,)),
            dma((NH, NK)), dma((NH, NK)),
            dma((NH, NX)), dma((NH, NX)),
            dma((8,)), dma((8,)),
        ],
        compiler_params=pltpu.CompilerParams(collective_id=0, has_side_effects=True),
    )(sinogram, detector_coord)


def solution(mesh):
    in_specs = (P("sl", "ang", None), P("ang", "sl", None))
    out_specs = P("ang", "sl", None)
    return jax.shard_map(shards, mesh=mesh, in_specs=in_specs, out_specs=out_specs, check_vma=False)
```

```python
import math

import jax
import jax.numpy as jnp
from jax import lax
from jax.experimental import pallas as pl
from jax.experimental.pallas import tpu as pltpu
from jax.sharding import PartitionSpec as P

MESH = pl.DeviceIdType.MESH
NY, NZ, NC, NH, NX = 4, 4, 2, 2, 4
NK = NY * NC


def flip(bit, by):
    return bit + by - 2 * bit * by


def lane_gather(table, lanes):
    return jnp.take_along_axis(table, lanes, axis=1, mode="promise_in_bounds")


def write_ramp(g_ref):
    depth, width = g_ref.shape

    def chunk(step, carry):
        base = pl.multiple_of(step * 16, 16)
        for lane in range(0, width, 256):
            row = lax.broadcasted_iota(jnp.int32, (16, 256), 0) + base
            column = lax.broadcasted_iota(jnp.int32, (16, 256), 1) + (lane - 768)
            offset = column - row
            real = offset.astype(jnp.float32)
            square = jnp.maximum(real * real, jnp.float32(1.0))
            odd = (offset & 1) != 0
            value = jnp.where(odd, jnp.float32(-1.0 / math.pi**2) / square, jnp.float32(0.0))
            value = jnp.where(offset == 0, jnp.float32(0.25), value)
            g_ref[pl.ds(base, 16), lane : lane + 256] = value.astype(jnp.bfloat16)
        return carry

    lax.fori_loop(0, depth // 16, chunk, 0)


def kernel(
    x_ref, c_ref, o_ref,
    csend, hbuf, sbuf, cbuf, g_ref, f_ref, t_ref, sc_ref, obuf, rbuf,
    s_send, s_recv, h_send, h_recv, c_send, c_recv, o_send, o_recv,
):
    ang, sl = lax.axis_index("ang"), lax.axis_index("sl")
    y, z, c = ang // 8, (ang // 2) % 4, ang % 2
    h, x = sl // 4, sl % 4

    def device(yy, zz, cc, hh, xx):
        return (yy * 8 + zz * 2 + cc, hh * 4 + xx)

    def near(dy, dc, dx):
        return device((y + dy) % NY, z, flip(c, dc), h, (x + dx) % NX)

    plane = [(dy, dc, dx) for dx in range(NX) for dy in range(NY) for dc in range(NC)][1:]
    across = device(y, z, c, flip(h, 1), x)
    owners = []
    for dh in range(NH):
        for dx in range(NX):
            block = flip(h, dh) * NX + (x - dx) % NX
            owners.append((4 * block + y, sl))
    sources = [((ang % 4) * 8 + zz * 2 + cc, sl) for zz in range(NZ) for cc in range(NC)]

    barrier = pltpu.get_barrier_semaphore()
    group = [near(*step) for step in plane] + [across]
    group += [device(y, (z + dz) % NZ, flip(c, dc), h, x) for dz in range(1, NZ) for dc in range(NC)]
    for other in group:
        pl.semaphore_signal(barrier, inc=1, device_id=other, device_id_type=MESH)
    for a in range(2):
        for p in range(4):
            csend[:, a, p, :] = c_ref[a, :, 128 * p : 128 * (p + 1)]
    pl.semaphore_wait(barrier, len(group))

    over = pltpu.make_async_remote_copy(
        src_ref=csend, dst_ref=hbuf, send_sem=h_send, recv_sem=h_recv,
        device_id=across, device_id_type=MESH,
    )
    over.start()

    def spread(block, dh):
        copies = []
        for dy, dc, dx in plane:
            k = dy * NC + dc
            row = 2 * ((y + dy) % NY) + flip(c, dc)
            copy = pltpu.make_async_remote_copy(
                src_ref=block.at[row],
                dst_ref=cbuf.at[k, :, dh * NX + dx],
                send_sem=c_send.at[dh, k, dx],
                recv_sem=c_recv.at[dh, k, dx],
                device_id=near(dy, dc, dx),
                device_id_type=MESH,
            )
            copy.start()
            copies.append(copy)
        cbuf[0, :, dh * NX, :, :] = block[2 * y + c]
        return copies

    passed = {0: spread(csend, 0)}
    sino = []
    for dy in range(NY):
        for dc in range(NC):
            k = dy * NC + dc
            if k == 0:
                sbuf[0] = x_ref[...]
                continue
            copy = pltpu.make_async_remote_copy(
                src_ref=x_ref,
                dst_ref=sbuf.at[k],
                send_sem=s_send.at[k],
                recv_sem=s_recv.at[k],
                device_id=near(dy, dc, 0),
                device_id_type=MESH,
            )
            copy.start()
            sino.append(copy)

    write_ramp(g_ref)

    over.wait_recv()
    passed[1] = spread(hbuf, 1)

    for copy in sino:
        copy.wait_recv()
    lhs = sbuf[...].reshape(NK * 16, 1024)
    for n in range(4):
        total = None
        for m in range(4):
            at = 768 - 256 * m + 256 * n
            part = jnp.dot(
                lhs[:, 256 * m : 256 * (m + 1)], g_ref[:, at : at + 256],
                preferred_element_type=jnp.float32,
            )
            total = part if total is None else total + part
        f_ref[2 * n] = total[:, :128]
        f_ref[2 * n + 1] = total[:, 128:]

    def pack(k, carry):
        for a in range(2):
            rows = pl.ds(k * 16 + a, 8, stride=2)
            value = jnp.concatenate([f_ref[n, rows, :] for n in range(8)], axis=1)
            top = jnp.maximum(jnp.max(jnp.abs(value), axis=1, keepdims=True), jnp.float32(1e-30))
            fixed = (value * (jnp.float32(32767.0) / top) + jnp.float32(32768.5)).astype(jnp.int32)
            fixed = fixed - 32768
            after = pltpu.roll(fixed, 1023, 1)
            t_ref[k, a] = (fixed << 16) | (after & 0xFFFF)
            sc_ref[k, a] = jnp.broadcast_to(top * jnp.float32(1.0 / 32767.0), (8, 128))
        return carry

    lax.fori_loop(0, NK, pack, 0)

    own = z * NC + c
    sent = []
    for dh in range(NH):
        for copy in passed[dh]:
            copy.wait_recv()

        def source(k, sums, dh=dh):
            sums = list(sums)
            for a in range(2):
                table = [t_ref[k, a, :, 128 * n : 128 * (n + 1)] for n in range(8)]
                scale = sc_ref[k, a]
                for dx in range(NX):
                    for p in range(4):
                        coord = cbuf[k, a, dh * NX + dx, p : p + 1, :]
                        coord = jnp.broadcast_to(coord, (8, 128))
                        left = coord >> 20
                        fraction = (coord & 0xFFFFF).astype(jnp.float32)
                        fraction = fraction * jnp.float32(1.0 / 1048576.0)
                        lanes = left & 127
                        found = [lane_gather(part, lanes) for part in table]
                        for bit in (128, 256, 512):
                            on = (left & bit) != 0
                            found = [
                                jnp.where(on, found[i + 1], found[i])
                                for i in range(0, len(found), 2)
                            ]
                        word = found[0]
                        low = (word >> 16).astype(jnp.float32)
                        high = ((word << 16) >> 16).astype(jnp.float32)
                        value = low + (high - low) * fraction
                        at = dx * 4 + p
                        sums[at] = sums[at] + value * scale
            return tuple(sums)

        zero = jnp.zeros((8, 128), jnp.float32)
        sums = lax.fori_loop(0, NK, source, (zero,) * 16)
        for dx in range(NX):
            slot = dh * NX + dx
            for p in range(4):
                obuf[slot, :, 128 * p : 128 * (p + 1)] = sums[dx * 4 + p].astype(jnp.bfloat16)
            copy = pltpu.make_async_remote_copy(
                src_ref=obuf.at[slot],
                dst_ref=rbuf.at[own],
                send_sem=o_send.at[slot],
                recv_sem=o_recv.at[own],
                device_id=owners[slot],
                device_id_type=MESH,
            )
            mine = owners[slot][0] == ang

            @pl.when(jnp.logical_not(mine))
            def _():
                copy.start()

            @pl.when(mine)
            def _():
                rbuf[own] = obuf[slot]

            sent.append((copy, mine))

    for at, source_device in enumerate(sources):
        arrival = pltpu.make_async_remote_copy(
            src_ref=obuf.at[0],
            dst_ref=rbuf.at[at],
            send_sem=o_send.at[0],
            recv_sem=o_recv.at[at],
            device_id=source_device,
            device_id_type=MESH,
        )

        @pl.when(source_device[0] != ang)
        def _():
            arrival.wait_recv()

    for cc in range(NC):
        total = rbuf[cc].astype(jnp.float32)
        for zz in range(1, NZ):
            total = total + rbuf[zz * NC + cc].astype(jnp.float32)
        o_ref[cc] = total * jnp.float32(math.pi / 64)

    for copy, mine in sent:

        @pl.when(jnp.logical_not(mine))
        def _():
            copy.wait_send()

    for copy in [over, *sino, *passed[0], *passed[1]]:
        copy.wait_send()


def shards(sinogram, detector_coord):
    dma = pltpu.SemaphoreType.DMA
    vmem = pl.BlockSpec(memory_space=pltpu.VMEM)
    return pl.pallas_call(
        kernel,
        out_shape=jax.ShapeDtypeStruct((2, 8, 512), jnp.float32),
        in_specs=[vmem, vmem],
        out_specs=vmem,
        scratch_shapes=[
            pltpu.VMEM((8, 2, 4, 128), jnp.int32),
            pltpu.VMEM((8, 2, 4, 128), jnp.int32),
            pltpu.VMEM((NK, 8, 2, 1024), jnp.bfloat16),
            pltpu.VMEM((NK, 2, 8, 4, 128), jnp.int32),
            pltpu.VMEM((256, 1792), jnp.bfloat16),
            pltpu.VMEM((8, NK * 16, 128), jnp.float32),
            pltpu.VMEM((NK, 2, 8, 1024), jnp.int32),
            pltpu.VMEM((NK, 2, 8, 128), jnp.float32),
            pltpu.VMEM((8, 8, 512), jnp.bfloat16),
            pltpu.VMEM((8, 8, 512), jnp.bfloat16),
            dma((NK,)), dma((NK,)),
            dma(()), dma(()),
            dma((NH, NK, NX)), dma((NH, NK, NX)),
            dma((8,)), dma((8,)),
        ],
        compiler_params=pltpu.CompilerParams(collective_id=0, has_side_effects=True),
    )(sinogram, detector_coord)


def solution(mesh):
    in_specs = (P("sl", "ang", None), P("ang", "sl", None))
    out_specs = P("ang", "sl", None)
    return jax.shard_map(shards, mesh=mesh, in_specs=in_specs, out_specs=out_specs, check_vma=False)
```

```python
import math

import jax
import jax.numpy as jnp
from jax import lax
from jax.experimental import pallas as pl
from jax.experimental.pallas import tpu as pltpu
from jax.sharding import PartitionSpec as P

MESH = pl.DeviceIdType.MESH
NY, NZ, NC, NH, NX = 4, 4, 2, 2, 4
NK = NY * NC
NB, STEP = 9, 127


def flip(bit, by):
    return bit + by - 2 * bit * by


def write_ramp(g_ref):
    depth, width = g_ref.shape

    def chunk(step, carry):
        base = pl.multiple_of(step * 16, 16)
        for lane in range(0, width, 256):
            row = lax.broadcasted_iota(jnp.int32, (16, 256), 0) + base
            column = lax.broadcasted_iota(jnp.int32, (16, 256), 1) + (lane - 768)
            offset = column - row
            real = offset.astype(jnp.float32)
            square = jnp.maximum(real * real, jnp.float32(1.0))
            odd = (offset & 1) != 0
            value = jnp.where(odd, jnp.float32(-1.0 / math.pi**2) / square, jnp.float32(0.0))
            value = jnp.where(offset == 0, jnp.float32(0.25), value)
            g_ref[pl.ds(base, 16), lane : lane + 256] = value.astype(jnp.bfloat16)
        return carry

    lax.fori_loop(0, depth // 16, chunk, 0)


def interpolate(block_values, coord, bins):
    left = coord >> 20
    fraction = (coord & 0xFFFFF).astype(jnp.float32) * jnp.float32(1.0 / 1048576.0)
    block = (left * 8257) >> 20
    within = (left - block * STEP).astype(jnp.float32)

    def rows(value):
        pair = jnp.concatenate([value, value], axis=0).astype(jnp.bfloat16)
        return jnp.concatenate([pair] * 8, axis=0)

    right = jnp.where(bins == rows(within + 1.0), rows(fraction), jnp.zeros((), jnp.bfloat16))
    weights = jnp.where(bins == rows(within), rows(1.0 - fraction), right)
    product = jnp.dot(block_values, weights, preferred_element_type=jnp.float32)
    low, high = product[0:8], product[8:16]
    for n in range(1, NB):
        here = block == n
        low = jnp.where(here, product[16 * n : 16 * n + 8], low)
        high = jnp.where(here, product[16 * n + 8 : 16 * n + 16], high)
    return low, high


def kernel(
    x_ref, c_ref, o_ref,
    csend, hbuf, sbuf, cbuf, g_ref, f_ref, v_ref, obuf,
    s_send, s_recv, h_send, h_recv, c_send, c_recv, o_send, o_recv, own_sem, tokens,
):
    ang, sl = lax.axis_index("ang"), lax.axis_index("sl")
    y, z, c = ang // 8, (ang // 2) % 4, ang % 2
    h, x = sl // 4, sl % 4
    x_high, x_low = x // 2, x % 2

    def device(yy, zz, cc, hh, xx):
        return (yy * 8 + zz * 2 + cc, hh * 4 + xx)

    def x_at(flip_high, flip_low):
        return flip(x_high, flip_high) * 2 + flip(x_low, flip_low)

    def near(dy, dc, high, low):
        return device((y + dy) % NY, z, flip(c, dc), h, x_at(high, low))

    across = device(y, z, c, flip(h, 1), x)
    twin, far_twin, sibling = near(0, 0, 0, 1), near(0, 0, 1, 0), near(0, 1, 0, 0)
    ring_y = [near(dy, 0, 0, 0) for dy in range(1, NY)]
    owners = []
    for dh in range(NH):
        for high in range(2):
            block = flip(h, dh) * NX + x_at(high, 0)
            for low in range(2):
                owners.append((4 * block + y, h * 4 + x_at(0, low)))
    row_x_low = (ang // 4) % 2
    source_sl = h * 4 + 2 * x_high + row_x_low
    sources = [((ang % 4) * 8 + zz * 2 + cc, source_sl) for zz in range(NZ) for cc in range(NC)]

    barrier = pltpu.get_barrier_semaphore()
    group = [across, twin, far_twin, *ring_y, sibling]
    group += [device(y, (z + dz) % NZ, c, h, x) for dz in range(1, NZ)]
    for other in group:
        pl.semaphore_signal(barrier, inc=1, device_id=other, device_id_type=MESH)
    for a in range(2):
        for p in range(4):
            csend[:, a, p, :] = c_ref[a, :, 128 * p : 128 * (p + 1)]
    sbuf[0] = x_ref[...]
    pl.semaphore_wait(barrier, len(group))

    over = pltpu.make_async_remote_copy(
        src_ref=csend, dst_ref=hbuf, send_sem=h_send, recv_sem=h_recv,
        device_id=across, device_id_type=MESH,
    )
    over.start()

    sino = {}

    def share(source, dy, dc, low, other):
        k = (dy * NC + dc) * 2 + low
        copy = pltpu.make_async_remote_copy(
            src_ref=source,
            dst_ref=sbuf.at[k],
            send_sem=s_send.at[k],
            recv_sem=s_recv.at[k],
            device_id=other,
            device_id_type=MESH,
        )
        copy.start()
        sino[k] = copy

    for dy in range(1, NY):
        share(x_ref, dy, 0, 0, ring_y[dy - 1])
    share(x_ref, 0, 0, 1, twin)
    share(x_ref, 0, 1, 0, sibling)
    for other in (twin, far_twin):
        pl.semaphore_signal(tokens.at[0], inc=1, device_id=other, device_id_type=MESH)
    write_ramp(g_ref)
    pl.semaphore_wait(tokens.at[0], 2)
    pl.semaphore_signal(tokens.at[1], inc=1, device_id=sibling, device_id_type=MESH)
    for dy in range(1, NY):
        share(x_ref, dy, 0, 1, near(dy, 0, 0, 1))
    pl.semaphore_wait(tokens.at[1], 1)

    def spread(block, dh):
        copies = []
        for high in range(2):
            for dy in range(NY):
                for dc in range(NC):
                    k = dy * NC + dc
                    if (high, k) == (0, 0):
                        continue
                    row = 2 * ((y + dy) % NY) + flip(c, dc)
                    copy = pltpu.make_async_remote_copy(
                        src_ref=block.at[row],
                        dst_ref=cbuf.at[k, :, 2 * dh + high],
                        send_sem=c_send.at[dh, k, high],
                        recv_sem=c_recv.at[dh, k, high],
                        device_id=near(dy, dc, high, 0),
                        device_id_type=MESH,
                    )
                    copy.start()
                    copies.append(copy)
        cbuf[0, :, 2 * dh, :, :] = block[2 * y + c]
        return copies

    passed = {0: spread(csend, 0)}

    for dy in range(NY):
        for low in range(2):
            k = dy * NC * 2 + low
            if k:
                sino[k].wait_recv()
                share(sbuf.at[k], dy, 1, low, sibling)

    over.wait_recv()
    passed[1] = spread(hbuf, 1)

    for dy in range(NY):
        for low in range(2):
            sino[(dy * NC + 1) * 2 + low].wait_recv()

    def filter_half(part, carry):
        lhs = sbuf[pl.ds(part * 8, 8)].reshape(128, 1024)
        for n in range(4):
            total = None
            for m in range(4):
                at = 768 - 256 * m + 256 * n
                term = jnp.dot(
                    lhs[:, 256 * m : 256 * (m + 1)], g_ref[:, at : at + 256],
                    preferred_element_type=jnp.float32,
                )
                total = term if total is None else total + term
            at = pl.multiple_of(part * 128, 128)
            f_ref[2 * n, pl.ds(at, 128)] = total[:, :128]
            f_ref[2 * n + 1, pl.ds(at, 128)] = total[:, 128:]
        return carry

    lax.fori_loop(0, 2, filter_half, 0)

    def lay_out(k, carry):
        for a in range(2):
            wide = []
            for low in range(2):
                rows = pl.ds((2 * k + low) * 16 + a, 8, stride=2)
                wide.append([f_ref[n, rows, :] for n in range(8)])
            for n in range(NB):
                block = []
                for parts in wide:
                    if n == 0:
                        block.append(parts[0])
                        continue
                    pair = [parts[n - 1], parts[n] if n < 8 else jnp.zeros_like(parts[0])]
                    turned = [pltpu.roll(part, n, 1) for part in pair]
                    lane = lax.broadcasted_iota(jnp.int32, (8, 128), 1)
                    block.append(jnp.where(lane < n, turned[0], turned[1]))
                v_ref[k, a, 16 * n : 16 * (n + 1), :] = jnp.concatenate(block).astype(jnp.bfloat16)
        return carry

    lax.fori_loop(0, NK, lay_out, 0)

    bins = lax.broadcasted_iota(jnp.int32, (128, 256), 0).astype(jnp.float32).astype(jnp.bfloat16)
    own = z * NC + c
    sent = []
    for dh in range(NH):
        for copy in passed[dh]:
            copy.wait_recv()

        def source(k, sums, dh=dh):
            sums = list(sums)
            for a in range(2):
                values = v_ref[k, a]
                for high in range(2):
                    for q in range(2):
                        coord = [
                            jnp.broadcast_to(cbuf[k, a, 2 * dh + high, p : p + 1, :], (8, 128))
                            for p in (2 * q, 2 * q + 1)
                        ]
                        taps = interpolate(values, jnp.concatenate(coord, axis=1), bins)
                        for low in range(2):
                            at = (high * 2 + q) * 2 + low
                            sums[at] = sums[at] + taps[low]
            return tuple(sums)

        zero = jnp.zeros((8, 256), jnp.float32)
        sums = lax.fori_loop(0, NK, source, (zero,) * 8)
        for high in range(2):
            for low in range(2):
                slot = (dh * 2 + high) * 2 + low
                for q in range(2):
                    part = sums[(high * 2 + q) * 2 + low]
                    obuf[slot, :, 256 * q : 256 * (q + 1)] = part.astype(jnp.bfloat16)
                copy = pltpu.make_async_remote_copy(
                    src_ref=obuf.at[slot],
                    dst_ref=o_ref.at[own],
                    send_sem=o_send.at[slot],
                    recv_sem=o_recv.at[own],
                    device_id=owners[slot],
                    device_id_type=MESH,
                )
                mine = jnp.logical_and(owners[slot][0] == ang, owners[slot][1] == sl)
                keep = pltpu.make_async_copy(obuf.at[slot], o_ref.at[own], own_sem)

                @pl.when(jnp.logical_not(mine))
                def _():
                    copy.start()

                @pl.when(mine)
                def _():
                    keep.start()

                sent.append((copy, keep, mine))

    for copy in [over, *sino.values(), *passed[0], *passed[1]]:
        copy.wait_send()

    for copy, keep, mine in sent:

        @pl.when(jnp.logical_not(mine))
        def _():
            copy.wait_send()

        @pl.when(mine)
        def _():
            keep.wait()

    for at, other in enumerate(sources):
        arrival = pltpu.make_async_remote_copy(
            src_ref=obuf.at[0],
            dst_ref=o_ref.at[at],
            send_sem=o_send.at[0],
            recv_sem=o_recv.at[at],
            device_id=other,
            device_id_type=MESH,
        )

        @pl.when(jnp.logical_or(other[0] != ang, other[1] != sl))
        def _():
            arrival.wait_recv()


def shards(sinogram, detector_coord):
    dma = pltpu.SemaphoreType.DMA
    vmem = pl.BlockSpec(memory_space=pltpu.VMEM)
    partials = pl.pallas_call(
        kernel,
        out_shape=jax.ShapeDtypeStruct((NZ * NC, 8, 512), jnp.bfloat16),
        in_specs=[vmem, vmem],
        out_specs=pl.BlockSpec(memory_space=pl.ANY),
        scratch_shapes=[
            pltpu.VMEM((8, 2, 4, 128), jnp.int32),
            pltpu.VMEM((8, 2, 4, 128), jnp.int32),
            pltpu.VMEM((2 * NK, 8, 2, 1024), jnp.bfloat16),
            pltpu.VMEM((NK, 2, 4, 4, 128), jnp.int32),
            pltpu.VMEM((256, 1792), jnp.bfloat16),
            pltpu.VMEM((8, 2 * NK * 16, 128), jnp.float32),
            pltpu.VMEM((NK, 2, NB * 16, 128), jnp.bfloat16),
            pltpu.VMEM((8, 8, 512), jnp.bfloat16),
            dma((2 * NK,)), dma((2 * NK,)),
            dma(()), dma(()),
            dma((NH, NK, 2)), dma((NH, NK, 2)),
            dma((8,)), dma((8,)),
            dma(()),
            pltpu.SemaphoreType.REGULAR((2,)),
        ],
        compiler_params=pltpu.CompilerParams(collective_id=0, has_side_effects=True),
    )(sinogram, detector_coord)
    partials = partials.reshape(NZ, NC, 8, 512).astype(jnp.float32)
    return jnp.sum(partials, axis=0) * jnp.float32(math.pi / 64)


def solution(mesh):
    in_specs = (P("sl", "ang", None), P("ang", "sl", None))
    out_specs = P("ang", "sl", None)
    return jax.shard_map(shards, mesh=mesh, in_specs=in_specs, out_specs=out_specs, check_vma=False)
```

```python
import math

import jax
import jax.numpy as jnp
from jax import lax
from jax.experimental import pallas as pl
from jax.experimental.pallas import tpu as pltpu
from jax.sharding import PartitionSpec as P

MESH = pl.DeviceIdType.MESH
NY, NZ, NC, NH, NX = 4, 4, 2, 2, 4
NB, STEP = 9, 127


def flip(bit, by):
    return bit + by - 2 * bit * by


def write_ramp(g_ref):
    depth, width = g_ref.shape

    def chunk(step, carry):
        base = pl.multiple_of(step * 16, 16)
        for lane in range(0, width, 256):
            row = lax.broadcasted_iota(jnp.int32, (16, 256), 0) + base
            column = lax.broadcasted_iota(jnp.int32, (16, 256), 1) + (lane - 768)
            offset = column - row
            real = offset.astype(jnp.float32)
            square = jnp.maximum(real * real, jnp.float32(1.0))
            odd = (offset & 1) != 0
            value = jnp.where(odd, jnp.float32(-1.0 / math.pi**2) / square, jnp.float32(0.0))
            value = jnp.where(offset == 0, jnp.float32(0.25), value)
            g_ref[pl.ds(base, 16), lane : lane + 256] = value.astype(jnp.bfloat16)
        return carry

    lax.fori_loop(0, depth // 16, chunk, 0)


def interpolate(block_values, coord, bins):
    left = coord >> 20
    fraction = (coord & 0xFFFFF).astype(jnp.float32) * jnp.float32(1.0 / 1048576.0)
    block = (left * 8257) >> 20
    within = (left - block * STEP).astype(jnp.float32)

    def rows(value):
        pair = jnp.concatenate([value, value], axis=0).astype(jnp.bfloat16)
        return jnp.concatenate([pair] * 8, axis=0)

    right = jnp.where(bins == rows(within + 1.0), rows(fraction), jnp.zeros((), jnp.bfloat16))
    weights = jnp.where(bins == rows(within), rows(1.0 - fraction), right)
    product = jnp.dot(block_values, weights, preferred_element_type=jnp.float32)
    low, high = product[0:8], product[8:16]
    for n in range(1, NB):
        here = block == n
        low = jnp.where(here, product[16 * n : 16 * n + 8], low)
        high = jnp.where(here, product[16 * n + 8 : 16 * n + 16], high)
    return low, high


def kernel(
    x_ref, c_ref, o_ref,
    cin, csend, hbuf, sbuf, cbuf, g_ref, f_ref, v_ref, obuf,
    in_sem, s_send, s_recv, h_send, h_recv, c_send, c_recv, o_send, o_recv, own_sem, tokens,
):
    load_x = pltpu.make_async_copy(x_ref, sbuf.at[0], in_sem.at[0])
    load_c = pltpu.make_async_copy(c_ref, cin, in_sem.at[1])
    load_x.start()
    load_c.start()
    ang, sl = lax.axis_index("ang"), lax.axis_index("sl")
    y, z, c = ang // 8, (ang // 2) % 4, ang % 2
    h, x = sl // 4, sl % 4
    x_high, x_low = x // 2, x % 2

    def device(yy, zz, cc, hh, xx):
        return (yy * 8 + zz * 2 + cc, hh * 4 + xx)

    def x_at(flip_high, flip_low):
        return flip(x_high, flip_high) * 2 + flip(x_low, flip_low)

    def near(dy, high, low):
        return device((y + dy) % NY, z, c, h, x_at(high, low))

    across = device(y, z, c, flip(h, 1), x)
    sibling = device(y, z, flip(c, 1), h, x)
    far_twin = near(0, 1, 0)
    sharers = [(dy, low) for dy in range(NY) for low in range(2)][1:]
    owners = []
    for dh in range(NH):
        for high in range(2):
            block = flip(h, dh) * NX + x_at(high, 0)
            for low in range(2):
                owners.append((4 * block + y, h * 4 + x_at(0, low)))
    row_x_low = (ang // 4) % 2
    source_sl = h * 4 + 2 * x_high + row_x_low
    sources = [((ang % 4) * 8 + zz * 2 + cc, source_sl) for zz in range(NZ) for cc in range(NC)]

    barrier = pltpu.get_barrier_semaphore()
    group = [across, far_twin, sibling] + [near(dy, 0, low) for dy, low in sharers]
    group += [device(y, (z + dz) % NZ, c, h, x) for dz in range(1, NZ)]
    for other in group:
        pl.semaphore_signal(barrier, inc=1, device_id=other, device_id_type=MESH)
    load_c.wait()
    for a in range(2):
        for p in range(4):
            csend[:, a, p, :] = cin[a, :, 128 * p : 128 * (p + 1)]
    load_x.wait()
    pl.semaphore_wait(barrier, len(group))

    over = pltpu.make_async_remote_copy(
        src_ref=csend, dst_ref=hbuf, send_sem=h_send, recv_sem=h_recv,
        device_id=across, device_id_type=MESH,
    )
    over.start()

    sino = []
    for dy, low in sharers:
        k = dy * 2 + low
        copy = pltpu.make_async_remote_copy(
            src_ref=sbuf.at[0],
            dst_ref=sbuf.at[k],
            send_sem=s_send.at[k],
            recv_sem=s_recv.at[k],
            device_id=near(dy, 0, low),
            device_id_type=MESH,
        )
        copy.start()
        sino.append(copy)
    pl.semaphore_signal(tokens.at[0], inc=1, device_id=far_twin, device_id_type=MESH)
    write_ramp(g_ref)
    pl.semaphore_wait(tokens.at[0], 1)

    def spread(block, dh):
        copies = []
        for high in range(2):
            for dy in range(NY):
                rows = pl.ds(2 * ((y + dy) % NY), 2)
                if (high, dy) == (0, 0):
                    cbuf[0, 2 * dh] = block[rows]
                    continue
                copy = pltpu.make_async_remote_copy(
                    src_ref=block.at[rows],
                    dst_ref=cbuf.at[dy, 2 * dh + high],
                    send_sem=c_send.at[dh, dy, high],
                    recv_sem=c_recv.at[dh, dy, high],
                    device_id=near(dy, high, 0),
                    device_id_type=MESH,
                )
                copy.start()
                copies.append(copy)
        return copies

    passed = {0: spread(csend, 0)}
    over.wait_recv()
    passed[1] = spread(hbuf, 1)
    for copy in sino:
        copy.wait_recv()
    pl.semaphore_signal(tokens.at[1], inc=1, device_id=sibling, device_id_type=MESH)

    lhs = sbuf[...].reshape(128, 1024)
    for n in range(4):
        total = None
        for m in range(4):
            at = 768 - 256 * m + 256 * n
            term = jnp.dot(
                lhs[:, 256 * m : 256 * (m + 1)], g_ref[:, at : at + 256],
                preferred_element_type=jnp.float32,
            )
            total = term if total is None else total + term
        f_ref[2 * n] = total[:, :128]
        f_ref[2 * n + 1] = total[:, 128:]

    def lay_out(k, carry):
        for a in range(2):
            wide = []
            for low in range(2):
                rows = pl.ds((2 * k + low) * 16 + a, 8, stride=2)
                wide.append([f_ref[n, rows, :] for n in range(8)])
            for n in range(NB):
                block = []
                for parts in wide:
                    if n == 0:
                        block.append(parts[0])
                        continue
                    pair = [parts[n - 1], parts[n] if n < 8 else jnp.zeros_like(parts[0])]
                    turned = [pltpu.roll(part, n, 1) for part in pair]
                    lane = lax.broadcasted_iota(jnp.int32, (8, 128), 1)
                    block.append(jnp.where(lane < n, turned[0], turned[1]))
                v_ref[k, a, 16 * n : 16 * (n + 1), :] = jnp.concatenate(block).astype(jnp.bfloat16)
        return carry

    lax.fori_loop(0, NY, lay_out, 0)

    bins = lax.broadcasted_iota(jnp.int32, (128, 256), 0).astype(jnp.float32).astype(jnp.bfloat16)
    own = z * NC + c
    sent = []
    for dh in range(NH):
        for copy in passed[dh]:
            copy.wait_recv()
        for high in range(2):
            sums = {}
            for dy in range(NY):
                for a in range(2):
                    values = v_ref[dy, a]
                    for row in range(2):
                        for q in range(2):
                            coord = [
                                jnp.broadcast_to(
                                    cbuf[dy, 2 * dh + high, row, a, p : p + 1, :], (8, 128)
                                )
                                for p in (2 * q, 2 * q + 1)
                            ]
                            taps = interpolate(values, jnp.concatenate(coord, axis=1), bins)
                            for low in range(2):
                                at = (row, q, low)
                                sums[at] = sums[at] + taps[low] if at in sums else taps[low]
            if (dh, high) == (0, 0):
                pl.semaphore_wait(tokens.at[1], 1)
            for low in range(2):
                slot = (dh * 2 + high) * 2 + low
                for row in range(2):
                    for q in range(2):
                        part = sums[row, q, low].astype(jnp.bfloat16)
                        obuf[slot, row, :, 256 * q : 256 * (q + 1)] = part
                copy = pltpu.make_async_remote_copy(
                    src_ref=obuf.at[slot],
                    dst_ref=o_ref.at[own],
                    send_sem=o_send.at[slot],
                    recv_sem=o_recv.at[own],
                    device_id=owners[slot],
                    device_id_type=MESH,
                )
                mine = jnp.logical_and(owners[slot][0] == ang, owners[slot][1] == sl)
                keep = pltpu.make_async_copy(obuf.at[slot], o_ref.at[own], own_sem)

                @pl.when(jnp.logical_not(mine))
                def _():
                    copy.start()

                @pl.when(mine)
                def _():
                    keep.start()

                sent.append((copy, keep, mine))

    for copy in [over, *sino, *passed[0], *passed[1]]:
        copy.wait_send()

    for copy, keep, mine in sent:

        @pl.when(jnp.logical_not(mine))
        def _():
            copy.wait_send()

        @pl.when(mine)
        def _():
            keep.wait()

    for at, other in enumerate(sources):
        arrival = pltpu.make_async_remote_copy(
            src_ref=obuf.at[0],
            dst_ref=o_ref.at[at],
            send_sem=o_send.at[0],
            recv_sem=o_recv.at[at],
            device_id=other,
            device_id_type=MESH,
        )

        @pl.when(jnp.logical_or(other[0] != ang, other[1] != sl))
        def _():
            arrival.wait_recv()


def shards(sinogram, detector_coord):
    dma = pltpu.SemaphoreType.DMA
    anywhere = pl.BlockSpec(memory_space=pl.ANY)
    partials = pl.pallas_call(
        kernel,
        out_shape=jax.ShapeDtypeStruct((NZ * NC, 2, 8, 512), jnp.bfloat16),
        in_specs=[anywhere, anywhere],
        out_specs=anywhere,
        scratch_shapes=[
            pltpu.VMEM((2, 8, 512), jnp.int32),
            pltpu.VMEM((8, 2, 4, 128), jnp.int32),
            pltpu.VMEM((8, 2, 4, 128), jnp.int32),
            pltpu.VMEM((2 * NY, 8, 2, 1024), jnp.bfloat16),
            pltpu.VMEM((NY, 4, 2, 2, 4, 128), jnp.int32),
            pltpu.VMEM((256, 1792), jnp.bfloat16),
            pltpu.VMEM((8, 128, 128), jnp.float32),
            pltpu.VMEM((NY, 2, NB * 16, 128), jnp.bfloat16),
            pltpu.VMEM((8, 2, 8, 512), jnp.bfloat16),
            dma((2,)),
            dma((2 * NY,)), dma((2 * NY,)),
            dma(()), dma(()),
            dma((NH, NY, 2)), dma((NH, NY, 2)),
            dma((8,)), dma((8,)),
            dma(()),
            pltpu.SemaphoreType.REGULAR((2,)),
        ],
        compiler_params=pltpu.CompilerParams(collective_id=0, has_side_effects=True),
    )(sinogram, detector_coord)
    total = partials[0].astype(jnp.float32)
    for part in range(1, NZ * NC):
        total = total + partials[part].astype(jnp.float32)
    return total * jnp.float32(math.pi / 64)


def solution(mesh):
    in_specs = (P("sl", "ang", None), P("ang", "sl", None))
    out_specs = P("ang", "sl", None)
    return jax.shard_map(shards, mesh=mesh, in_specs=in_specs, out_specs=out_specs, check_vma=False)
```

```python
import math

import jax
import jax.numpy as jnp
from jax import lax
from jax.experimental import pallas as pl
from jax.experimental.pallas import tpu as pltpu
from jax.sharding import PartitionSpec as P

MESH = pl.DeviceIdType.MESH
NY, NZ, NC, NH, NX = 4, 4, 2, 2, 4
NB, STEP = 9, 127


def flip(bit, by):
    return bit + by - 2 * bit * by


def write_ramp(g_ref):
    depth, width = g_ref.shape

    def chunk(step, carry):
        base = pl.multiple_of(step * 16, 16)
        for lane in range(0, width, 256):
            row = lax.broadcasted_iota(jnp.int32, (16, 256), 0) + base
            column = lax.broadcasted_iota(jnp.int32, (16, 256), 1) + (lane - 768)
            offset = column - row
            real = offset.astype(jnp.float32)
            square = jnp.maximum(real * real, jnp.float32(1.0))
            odd = (offset & 1) != 0
            value = jnp.where(odd, jnp.float32(-1.0 / math.pi**2) / square, jnp.float32(0.0))
            value = jnp.where(offset == 0, jnp.float32(0.25), value)
            g_ref[pl.ds(base, 16), lane : lane + 256] = value.astype(jnp.bfloat16)
        return carry

    lax.fori_loop(0, depth // 16, chunk, 0)


def interpolate(block_values, coord, bins):
    left = coord >> 20
    fraction = (coord & 0xFFFFF).astype(jnp.float32) * jnp.float32(1.0 / 1048576.0)
    block = (left * 8257) >> 20
    within = (left - block * STEP).astype(jnp.float32)

    def rows(value):
        pair = jnp.concatenate([value, value], axis=0).astype(jnp.bfloat16)
        return jnp.concatenate([pair] * 8, axis=0)

    right = jnp.where(bins == rows(within + 1.0), rows(fraction), jnp.zeros((), jnp.bfloat16))
    weights = jnp.where(bins == rows(within), rows(1.0 - fraction), right)
    product = jnp.dot(block_values, weights, preferred_element_type=jnp.float32)
    low, high = product[0:8], product[8:16]
    for n in range(1, NB):
        here = block == n
        low = jnp.where(here, product[16 * n : 16 * n + 8], low)
        high = jnp.where(here, product[16 * n + 8 : 16 * n + 16], high)
    return low, high


def kernel(
    x_ref, c_ref, o_ref,
    cin, csend, hbuf, sbuf, cbuf, g_ref, f_ref, v_ref, obuf,
    in_sem, s_send, s_recv, h_send, h_recv, c_send, c_recv, o_send, o_recv, own_sem, tokens,
):
    load_x = pltpu.make_async_copy(x_ref, sbuf.at[0], in_sem.at[0])
    load_c = pltpu.make_async_copy(c_ref, cin, in_sem.at[1])
    load_x.start()
    load_c.start()
    ang, sl = lax.axis_index("ang"), lax.axis_index("sl")
    y, z, c = ang // 8, (ang // 2) % 4, ang % 2
    h, x = sl // 4, sl % 4
    x_high, x_low = x // 2, x % 2

    def device(yy, zz, cc, hh, xx):
        return (yy * 8 + zz * 2 + cc, hh * 4 + xx)

    def x_at(flip_high, flip_low):
        return flip(x_high, flip_high) * 2 + flip(x_low, flip_low)

    def near(dy, high, low):
        return device((y + dy) % NY, z, c, h, x_at(high, low))

    across = device(y, z, c, flip(h, 1), x)
    sibling = device(y, z, flip(c, 1), h, x)
    far_twin = near(0, 1, 1)
    sharers = [(dy, low) for dy in range(NY) for low in range(2)][1:]
    def pair_of(yy, hh):
        return (yy + 2 * hh) % NY

    owners = []
    for dh in range(NH):
        for far in range(2):
            h_block = flip(h, dh)
            block = h_block * NX + x_at(far, far)
            for low in range(2):
                owners.append((4 * block + pair_of(y, h_block), h * 4 + x_at(0, low)))
    h_row, x_row = ang // 16, (ang // 4) % 4
    source_sl = h * 4 + 2 * x_high + flip(x_row % 2, flip(x_row // 2, x_high))
    source_y = pair_of(ang % 4, h_row)
    sources = [(source_y * 8 + zz * 2 + cc, source_sl) for zz in range(NZ) for cc in range(NC)]

    barrier = pltpu.get_barrier_semaphore()
    group = [across, far_twin, sibling] + [near(dy, 0, low) for dy, low in sharers]
    group += [device(y, (z + dz) % NZ, c, h, x) for dz in range(1, NZ)]
    for other in group:
        pl.semaphore_signal(barrier, inc=1, device_id=other, device_id_type=MESH)
    load_c.wait()
    for a in range(2):
        for p in range(4):
            csend[:, a, p, :] = cin[a, :, 128 * p : 128 * (p + 1)]
    load_x.wait()
    pl.semaphore_wait(barrier, len(group))

    over = pltpu.make_async_remote_copy(
        src_ref=csend, dst_ref=hbuf, send_sem=h_send, recv_sem=h_recv,
        device_id=across, device_id_type=MESH,
    )
    over.start()

    sino = []
    for dy, low in sharers:
        k = dy * 2 + low
        copy = pltpu.make_async_remote_copy(
            src_ref=sbuf.at[0],
            dst_ref=sbuf.at[k],
            send_sem=s_send.at[k],
            recv_sem=s_recv.at[k],
            device_id=near(dy, 0, low),
            device_id_type=MESH,
        )
        copy.start()
        sino.append(copy)
    pl.semaphore_signal(tokens.at[0], inc=1, device_id=far_twin, device_id_type=MESH)
    write_ramp(g_ref)
    pl.semaphore_wait(tokens.at[0], 1)

    def spread(block, dh):
        copies = []
        for high in range(2):
            for dy in range(NY):
                rows = pl.ds(2 * pair_of(y + dy, flip(h, dh)), 2)
                if (high, dy) == (0, 0):
                    cbuf[0, 2 * dh] = block[rows]
                    continue
                copy = pltpu.make_async_remote_copy(
                    src_ref=block.at[rows],
                    dst_ref=cbuf.at[dy, 2 * dh + high],
                    send_sem=c_send.at[dh, dy, high],
                    recv_sem=c_recv.at[dh, dy, high],
                    device_id=near(dy, high, high),
                    device_id_type=MESH,
                )
                copy.start()
                copies.append(copy)
        return copies

    passed = {0: spread(csend, 0)}
    over.wait_recv()
    passed[1] = spread(hbuf, 1)
    for copy in sino:
        copy.wait_recv()
    pl.semaphore_signal(tokens.at[1], inc=1, device_id=sibling, device_id_type=MESH)

    lhs = sbuf[...].reshape(128, 1024)
    for n in range(4):
        total = None
        for m in range(4):
            at = 768 - 256 * m + 256 * n
            term = jnp.dot(
                lhs[:, 256 * m : 256 * (m + 1)], g_ref[:, at : at + 256],
                preferred_element_type=jnp.float32,
            )
            total = term if total is None else total + term
        f_ref[2 * n] = total[:, :128]
        f_ref[2 * n + 1] = total[:, 128:]

    def lay_out(k, carry):
        for a in range(2):
            wide = []
            for low in range(2):
                rows = pl.ds((2 * k + low) * 16 + a, 8, stride=2)
                wide.append([f_ref[n, rows, :] for n in range(8)])
            for n in range(NB):
                block = []
                for parts in wide:
                    if n == 0:
                        block.append(parts[0])
                        continue
                    pair = [parts[n - 1], parts[n] if n < 8 else jnp.zeros_like(parts[0])]
                    turned = [pltpu.roll(part, n, 1) for part in pair]
                    lane = lax.broadcasted_iota(jnp.int32, (8, 128), 1)
                    block.append(jnp.where(lane < n, turned[0], turned[1]))
                v_ref[k, a, 16 * n : 16 * (n + 1), :] = jnp.concatenate(block).astype(jnp.bfloat16)
        return carry

    lax.fori_loop(0, NY, lay_out, 0)

    bins = lax.broadcasted_iota(jnp.int32, (128, 256), 0).astype(jnp.float32).astype(jnp.bfloat16)
    own = z * NC + c
    sent = []
    for dh in range(NH):
        for copy in passed[dh]:
            copy.wait_recv()
        for high in range(2):
            sums = {}
            for dy in range(NY):
                for a in range(2):
                    values = v_ref[dy, a]
                    for row in range(2):
                        for q in range(2):
                            coord = [
                                jnp.broadcast_to(
                                    cbuf[dy, 2 * dh + high, row, a, p : p + 1, :], (8, 128)
                                )
                                for p in (2 * q, 2 * q + 1)
                            ]
                            taps = interpolate(values, jnp.concatenate(coord, axis=1), bins)
                            for low in range(2):
                                at = (row, q, low)
                                sums[at] = sums[at] + taps[low] if at in sums else taps[low]
            if (dh, high) == (0, 0):
                pl.semaphore_wait(tokens.at[1], 1)
            for low in range(2):
                slot = (dh * 2 + high) * 2 + low
                for row in range(2):
                    for q in range(2):
                        part = sums[row, q, low].astype(jnp.bfloat16)
                        obuf[slot, row, :, 256 * q : 256 * (q + 1)] = part
                copy = pltpu.make_async_remote_copy(
                    src_ref=obuf.at[slot],
                    dst_ref=o_ref.at[own],
                    send_sem=o_send.at[slot],
                    recv_sem=o_recv.at[own],
                    device_id=owners[slot],
                    device_id_type=MESH,
                )
                mine = jnp.logical_and(owners[slot][0] == ang, owners[slot][1] == sl)
                keep = pltpu.make_async_copy(obuf.at[slot], o_ref.at[own], own_sem)

                @pl.when(jnp.logical_not(mine))
                def _():
                    copy.start()

                @pl.when(mine)
                def _():
                    keep.start()

                sent.append((copy, keep, mine))

    for copy in [over, *sino, *passed[0], *passed[1]]:
        copy.wait_send()

    for copy, keep, mine in sent:

        @pl.when(jnp.logical_not(mine))
        def _():
            copy.wait_send()

        @pl.when(mine)
        def _():
            keep.wait()

    for at, other in enumerate(sources):
        arrival = pltpu.make_async_remote_copy(
            src_ref=obuf.at[0],
            dst_ref=o_ref.at[at],
            send_sem=o_send.at[0],
            recv_sem=o_recv.at[at],
            device_id=other,
            device_id_type=MESH,
        )

        @pl.when(jnp.logical_or(other[0] != ang, other[1] != sl))
        def _():
            arrival.wait_recv()


def shards(sinogram, detector_coord):
    dma = pltpu.SemaphoreType.DMA
    anywhere = pl.BlockSpec(memory_space=pl.ANY)
    partials = pl.pallas_call(
        kernel,
        out_shape=jax.ShapeDtypeStruct((NZ * NC, 2, 8, 512), jnp.bfloat16),
        in_specs=[anywhere, anywhere],
        out_specs=anywhere,
        scratch_shapes=[
            pltpu.VMEM((2, 8, 512), jnp.int32),
            pltpu.VMEM((8, 2, 4, 128), jnp.int32),
            pltpu.VMEM((8, 2, 4, 128), jnp.int32),
            pltpu.VMEM((2 * NY, 8, 2, 1024), jnp.bfloat16),
            pltpu.VMEM((NY, 4, 2, 2, 4, 128), jnp.int32),
            pltpu.VMEM((256, 1792), jnp.bfloat16),
            pltpu.VMEM((8, 128, 128), jnp.float32),
            pltpu.VMEM((NY, 2, NB * 16, 128), jnp.bfloat16),
            pltpu.VMEM((8, 2, 8, 512), jnp.bfloat16),
            dma((2,)),
            dma((2 * NY,)), dma((2 * NY,)),
            dma(()), dma(()),
            dma((NH, NY, 2)), dma((NH, NY, 2)),
            dma((8,)), dma((8,)),
            dma(()),
            pltpu.SemaphoreType.REGULAR((2,)),
        ],
        compiler_params=pltpu.CompilerParams(collective_id=0, has_side_effects=True),
    )(sinogram, detector_coord)
    total = partials[0].astype(jnp.float32)
    for part in range(1, NZ * NC):
        total = total + partials[part].astype(jnp.float32)
    return total * jnp.float32(math.pi / 64)


def solution(mesh):
    in_specs = (P("sl", "ang", None), P("ang", "sl", None))
    out_specs = P("ang", "sl", None)
    return jax.shard_map(shards, mesh=mesh, in_specs=in_specs, out_specs=out_specs, check_vma=False)
```

```python
import math

import jax
import jax.numpy as jnp
from jax import lax
from jax.experimental import pallas as pl
from jax.experimental.pallas import tpu as pltpu
from jax.sharding import PartitionSpec as P

MESH = pl.DeviceIdType.MESH
NY, NZ, NC, NH, NX = 4, 4, 2, 2, 4
NB, STEP = 9, 127


def flip(bit, by):
    return bit + by - 2 * bit * by


def write_ramp(g_ref):
    depth, width = g_ref.shape

    def chunk(step, carry):
        base = pl.multiple_of(step * 16, 16)
        for lane in range(0, width, 256):
            row = lax.broadcasted_iota(jnp.int32, (16, 256), 0) + base
            column = lax.broadcasted_iota(jnp.int32, (16, 256), 1) + (lane - 768)
            offset = column - row
            real = offset.astype(jnp.float32)
            square = jnp.maximum(real * real, jnp.float32(1.0))
            odd = (offset & 1) != 0
            value = jnp.where(odd, jnp.float32(-1.0 / math.pi**2) / square, jnp.float32(0.0))
            value = jnp.where(offset == 0, jnp.float32(0.25), value)
            g_ref[pl.ds(base, 16), lane : lane + 256] = value.astype(jnp.bfloat16)
        return carry

    lax.fori_loop(0, depth // 16, chunk, 0)


def interpolate(block_values, coord, bins):
    left = coord >> 20
    fraction = (coord & 0xFFFFF).astype(jnp.float32) * jnp.float32(1.0 / 1048576.0)
    block = (left * 8257) >> 20
    within = (left - block * STEP).astype(jnp.float32)

    def rows(value):
        pair = jnp.concatenate([value, value], axis=0).astype(jnp.bfloat16)
        return jnp.concatenate([pair] * 8, axis=0)

    right = jnp.where(bins == rows(within + 1.0), rows(fraction), jnp.zeros((), jnp.bfloat16))
    weights = jnp.where(bins == rows(within), rows(1.0 - fraction), right)
    product = jnp.dot(block_values, weights, preferred_element_type=jnp.float32)
    low, high = product[0:8], product[8:16]
    for n in range(1, NB):
        here = block == n
        low = jnp.where(here, product[16 * n : 16 * n + 8], low)
        high = jnp.where(here, product[16 * n + 8 : 16 * n + 16], high)
    return low, high


def kernel(
    x_ref, c_ref, o_ref,
    cin, csend, hbuf, sbuf, cbuf, g_ref, f_ref, v_ref, obuf,
    in_sem, s_send, s_recv, h_send, h_recv, c_send, c_recv, o_send, o_recv, own_sem, tokens,
):
    load_x = pltpu.make_async_copy(x_ref, sbuf.at[0], in_sem.at[0])
    load_c = pltpu.make_async_copy(c_ref, cin, in_sem.at[1])
    load_x.start()
    load_c.start()
    ang, sl = lax.axis_index("ang"), lax.axis_index("sl")
    y, z, c = ang // 8, (ang // 2) % 4, ang % 2
    h, x = sl // 4, sl % 4
    x_high, x_low = x // 2, x % 2

    def device(yy, zz, cc, hh, xx):
        return (yy * 8 + zz * 2 + cc, hh * 4 + xx)

    def x_at(flip_high, flip_low):
        return flip(x_high, flip_high) * 2 + flip(x_low, flip_low)

    def near(dy, high, low):
        return device((y + dy) % NY, z, c, h, x_at(high, low))

    across = device(y, z, c, flip(h, 1), x)
    sibling = device(y, z, flip(c, 1), h, x)
    far_twin = near(0, 1, 1)
    sharers = [(dy, low) for dy in range(NY) for low in range(2)][1:]
    def pair_of(yy, hh):
        return (yy + 2 * hh) % NY

    owners = []
    for dh in range(NH):
        for far in range(2):
            h_block = flip(h, dh)
            block = h_block * NX + x_at(far, far)
            for low in range(2):
                owners.append((4 * block + pair_of(y, h_block), h * 4 + x_at(0, low)))
    h_row, x_row = ang // 16, (ang // 4) % 4
    source_sl = h * 4 + 2 * x_high + flip(x_row % 2, flip(x_row // 2, x_high))
    source_y = pair_of(ang % 4, h_row)
    sources = [(source_y * 8 + zz * 2 + cc, source_sl) for zz in range(NZ) for cc in range(NC)]

    barrier = pltpu.get_barrier_semaphore()
    group = [across, far_twin, sibling] + [near(dy, 0, low) for dy, low in sharers]
    group += [device(y, (z + dz) % NZ, c, h, x) for dz in range(1, NZ)]
    for other in group:
        pl.semaphore_signal(barrier, inc=1, device_id=other, device_id_type=MESH)
    load_c.wait()
    for a in range(2):
        for p in range(4):
            csend[:, a, p, :] = cin[a, :, 128 * p : 128 * (p + 1)]
    load_x.wait()
    pl.semaphore_wait(barrier, len(group))

    over = pltpu.make_async_remote_copy(
        src_ref=csend, dst_ref=hbuf, send_sem=h_send, recv_sem=h_recv,
        device_id=across, device_id_type=MESH,
    )
    over.start()

    sino = []
    for dy, low in sharers:
        k = dy * 2 + low
        copy = pltpu.make_async_remote_copy(
            src_ref=sbuf.at[0],
            dst_ref=sbuf.at[k],
            send_sem=s_send.at[k],
            recv_sem=s_recv.at[k],
            device_id=near(dy, 0, low),
            device_id_type=MESH,
        )
        copy.start()
        sino.append(copy)
    pl.semaphore_signal(tokens.at[0], inc=1, device_id=far_twin, device_id_type=MESH)
    write_ramp(g_ref)
    pl.semaphore_wait(tokens.at[0], 1)

    def spread(block, dh):
        copies = {}
        for far in range(2):
            for dy in range(NY):
                rows = pl.ds(2 * pair_of(y + dy, flip(h, dh)), 2)
                if (far, dy) == (0, 0):
                    cbuf[0, 2 * dh] = block[rows]
                    continue
                copy = pltpu.make_async_remote_copy(
                    src_ref=block.at[rows],
                    dst_ref=cbuf.at[dy, 2 * dh + far],
                    send_sem=c_send.at[dh, dy, far],
                    recv_sem=c_recv.at[dh, dy, far],
                    device_id=near(dy, far, far),
                    device_id_type=MESH,
                )
                copy.start()
                copies[far, dy] = copy
        return copies

    passed = {0: spread(csend, 0)}
    over.wait_recv()
    passed[1] = spread(hbuf, 1)
    for copy in sino:
        copy.wait_recv()
    pl.semaphore_signal(tokens.at[1], inc=1, device_id=sibling, device_id_type=MESH)

    lhs = sbuf[...].reshape(128, 1024)
    for n in range(4):
        total = None
        for m in range(4):
            at = 768 - 256 * m + 256 * n
            term = jnp.dot(
                lhs[:, 256 * m : 256 * (m + 1)], g_ref[:, at : at + 256],
                preferred_element_type=jnp.float32,
            )
            total = term if total is None else total + term
        f_ref[2 * n] = total[:, :128]
        f_ref[2 * n + 1] = total[:, 128:]

    def lay_out(k, carry):
        for a in range(2):
            wide = []
            for low in range(2):
                rows = pl.ds((2 * k + low) * 16 + a, 8, stride=2)
                wide.append([f_ref[n, rows, :] for n in range(8)])
            for n in range(NB):
                block = []
                for parts in wide:
                    if n == 0:
                        block.append(parts[0])
                        continue
                    pair = [parts[n - 1], parts[n] if n < 8 else jnp.zeros_like(parts[0])]
                    turned = [pltpu.roll(part, n, 1) for part in pair]
                    lane = lax.broadcasted_iota(jnp.int32, (8, 128), 1)
                    block.append(jnp.where(lane < n, turned[0], turned[1]))
                v_ref[k, a, 16 * n : 16 * (n + 1), :] = jnp.concatenate(block).astype(jnp.bfloat16)
        return carry

    lax.fori_loop(0, NY, lay_out, 0)

    bins = lax.broadcasted_iota(jnp.int32, (128, 256), 0).astype(jnp.float32).astype(jnp.bfloat16)
    own = z * NC + c
    sent = []
    for dh in range(NH):
        for high in range(2):
            for dy in range(NY):
                if (high, dy) in passed[dh]:
                    passed[dh][high, dy].wait_recv()
            sums = {}
            for dy in range(NY):
                for a in range(2):
                    values = v_ref[dy, a]
                    for row in range(2):
                        for q in range(2):
                            coord = [
                                jnp.broadcast_to(
                                    cbuf[dy, 2 * dh + high, row, a, p : p + 1, :], (8, 128)
                                )
                                for p in (2 * q, 2 * q + 1)
                            ]
                            taps = interpolate(values, jnp.concatenate(coord, axis=1), bins)
                            for low in range(2):
                                at = (row, q, low)
                                sums[at] = sums[at] + taps[low] if at in sums else taps[low]
            if (dh, high) == (0, 0):
                pl.semaphore_wait(tokens.at[1], 1)
            for low in range(2):
                slot = (dh * 2 + high) * 2 + low
                for q in range(2):
                    both = jnp.concatenate([sums[0, q, low], sums[1, q, low]], axis=0)
                    both = (both * jnp.float32(math.pi / 64)).astype(jnp.bfloat16)
                    obuf[slot, :, 256 * q : 256 * (q + 1)] = both
                copy = pltpu.make_async_remote_copy(
                    src_ref=obuf.at[slot],
                    dst_ref=o_ref.at[own],
                    send_sem=o_send.at[slot],
                    recv_sem=o_recv.at[own],
                    device_id=owners[slot],
                    device_id_type=MESH,
                )
                mine = jnp.logical_and(owners[slot][0] == ang, owners[slot][1] == sl)
                keep = pltpu.make_async_copy(obuf.at[slot], o_ref.at[own], own_sem)

                @pl.when(jnp.logical_not(mine))
                def _():
                    copy.start()

                @pl.when(mine)
                def _():
                    keep.start()

                sent.append((copy, keep, mine))

    for copy in [over, *sino, *passed[0].values(), *passed[1].values()]:
        copy.wait_send()

    for copy, keep, mine in sent:

        @pl.when(jnp.logical_not(mine))
        def _():
            copy.wait_send()

        @pl.when(mine)
        def _():
            keep.wait()

    for at, other in enumerate(sources):
        arrival = pltpu.make_async_remote_copy(
            src_ref=obuf.at[0],
            dst_ref=o_ref.at[at],
            send_sem=o_send.at[0],
            recv_sem=o_recv.at[at],
            device_id=other,
            device_id_type=MESH,
        )

        @pl.when(jnp.logical_or(other[0] != ang, other[1] != sl))
        def _():
            arrival.wait_recv()


def shards(sinogram, detector_coord):
    dma = pltpu.SemaphoreType.DMA
    anywhere = pl.BlockSpec(memory_space=pl.ANY)
    partials = pl.pallas_call(
        kernel,
        out_shape=jax.ShapeDtypeStruct((NZ * NC, 16, 512), jnp.bfloat16),
        in_specs=[anywhere, anywhere],
        out_specs=anywhere,
        scratch_shapes=[
            pltpu.VMEM((2, 8, 512), jnp.int32),
            pltpu.VMEM((8, 2, 4, 128), jnp.int32),
            pltpu.VMEM((8, 2, 4, 128), jnp.int32),
            pltpu.VMEM((2 * NY, 8, 2, 1024), jnp.bfloat16),
            pltpu.VMEM((NY, 4, 2, 2, 4, 128), jnp.int32),
            pltpu.VMEM((256, 1792), jnp.bfloat16),
            pltpu.VMEM((8, 128, 128), jnp.float32),
            pltpu.VMEM((NY, 2, NB * 16, 128), jnp.bfloat16),
            pltpu.VMEM((8, 16, 512), jnp.bfloat16),
            dma((2,)),
            dma((2 * NY,)), dma((2 * NY,)),
            dma(()), dma(()),
            dma((NH, NY, 2)), dma((NH, NY, 2)),
            dma((8,)), dma((8,)),
            dma(()),
            pltpu.SemaphoreType.REGULAR((2,)),
        ],
        compiler_params=pltpu.CompilerParams(collective_id=0, has_side_effects=True),
    )(sinogram, detector_coord)
    return jnp.sum(partials.astype(jnp.float32), axis=0).reshape(2, 8, 512)


def solution(mesh):
    in_specs = (P("sl", "ang", None), P("ang", "sl", None))
    out_specs = P("ang", "sl", None)
    return jax.shard_map(shards, mesh=mesh, in_specs=in_specs, out_specs=out_specs, check_vma=False)
```

```python
import math

import jax
import jax.numpy as jnp
from jax import lax
from jax.experimental import pallas as pl
from jax.experimental.pallas import tpu as pltpu
from jax.sharding import PartitionSpec as P

MESH = pl.DeviceIdType.MESH
NY, NZ, NC, NH, NX = 4, 4, 2, 2, 4
NB, STEP = 9, 127


def flip(bit, by):
    return bit + by - 2 * bit * by


def write_ramp(g_ref):
    depth, width = g_ref.shape

    def chunk(step, carry):
        base = pl.multiple_of(step * 16, 16)
        for lane in range(0, width, 256):
            row = lax.broadcasted_iota(jnp.int32, (16, 256), 0) + base
            column = lax.broadcasted_iota(jnp.int32, (16, 256), 1) + (lane - 768)
            offset = column - row
            real = offset.astype(jnp.float32)
            square = jnp.maximum(real * real, jnp.float32(1.0))
            odd = (offset & 1) != 0
            value = jnp.where(odd, jnp.float32(-1.0 / math.pi**2) / square, jnp.float32(0.0))
            value = jnp.where(offset == 0, jnp.float32(0.25), value)
            g_ref[pl.ds(base, 16), lane : lane + 256] = value.astype(jnp.bfloat16)
        return carry

    lax.fori_loop(0, depth // 16, chunk, 0)


def interpolate(block_values, coord, bins):
    left = coord >> 20
    fraction = (coord & 0xFFFFF).astype(jnp.float32) * jnp.float32(1.0 / 1048576.0)
    block = (left * 8257) >> 20
    within = (left - block * STEP).astype(jnp.float32)

    def rows(value):
        pair = jnp.concatenate([value, value], axis=0).astype(jnp.bfloat16)
        return jnp.concatenate([pair] * 8, axis=0)

    right = jnp.where(bins == rows(within + 1.0), rows(fraction), jnp.zeros((), jnp.bfloat16))
    weights = jnp.where(bins == rows(within), rows(1.0 - fraction), right)
    product = jnp.dot(block_values, weights, preferred_element_type=jnp.float32)
    low, high = product[0:8], product[8:16]
    for n in range(1, NB):
        here = block == n
        low = jnp.where(here, product[16 * n : 16 * n + 8], low)
        high = jnp.where(here, product[16 * n + 8 : 16 * n + 16], high)
    return low, high


def kernel(
    x_ref, c_ref, o_ref,
    cin, csend, hbuf, sbuf, cbuf, g_ref, f_ref, v_ref, obuf,
    in_sem, s_send, s_recv, h_send, h_recv, c_send, c_recv, o_send, o_recv, own_sem, tokens,
):
    load_x = pltpu.make_async_copy(x_ref, sbuf.at[0], in_sem.at[0])
    load_c = pltpu.make_async_copy(c_ref, cin, in_sem.at[1])
    load_x.start()
    load_c.start()
    ang, sl = lax.axis_index("ang"), lax.axis_index("sl")
    y, z, c = ang // 8, (ang // 2) % 4, ang % 2
    h, x = sl // 4, sl % 4
    x_high, x_low = x // 2, x % 2

    def device(yy, zz, cc, hh, xx):
        return (yy * 8 + zz * 2 + cc, hh * 4 + xx)

    def x_at(flip_high, flip_low):
        return flip(x_high, flip_high) * 2 + flip(x_low, flip_low)

    def near(dy, high, low):
        return device((y + dy) % NY, z, c, h, x_at(high, low))

    across = device(y, z, c, flip(h, 1), x)
    sibling = device(y, z, flip(c, 1), h, x)
    far_twin = near(0, 1, 1)
    sharers = [(dy, low) for dy in range(NY) for low in range(2)][1:]
    def pair_of(yy, hh):
        return (yy + 2 * hh) % NY

    owners = []
    for dh in range(NH):
        for far in range(2):
            h_block = flip(h, dh)
            block = h_block * NX + x_at(far, far)
            for low in range(2):
                owners.append((4 * block + pair_of(y, h_block), h * 4 + x_at(0, low)))
    h_row, x_row = ang // 16, (ang // 4) % 4
    source_sl = h * 4 + 2 * x_high + flip(x_row % 2, flip(x_row // 2, x_high))
    source_y = pair_of(ang % 4, h_row)
    sources = [(source_y * 8 + zz * 2 + cc, source_sl) for zz in range(NZ) for cc in range(NC)]

    barrier = pltpu.get_barrier_semaphore()
    group = [across, far_twin, sibling] + [near(dy, 0, low) for dy, low in sharers]
    group += [device(y, (z + dz) % NZ, c, h, x) for dz in range(1, NZ)]
    for other in group:
        pl.semaphore_signal(barrier, inc=1, device_id=other, device_id_type=MESH)
    load_c.wait()
    for a in range(2):
        for p in range(4):
            csend[:, a, p, :] = cin[a, :, 128 * p : 128 * (p + 1)]
    load_x.wait()
    pl.semaphore_wait(barrier, len(group))

    over = pltpu.make_async_remote_copy(
        src_ref=csend, dst_ref=hbuf, send_sem=h_send, recv_sem=h_recv,
        device_id=across, device_id_type=MESH,
    )
    over.start()

    sino = []
    for dy, low in sharers:
        k = dy * 2 + low
        copy = pltpu.make_async_remote_copy(
            src_ref=sbuf.at[0],
            dst_ref=sbuf.at[k],
            send_sem=s_send.at[k],
            recv_sem=s_recv.at[k],
            device_id=near(dy, 0, low),
            device_id_type=MESH,
        )
        copy.start()
        sino.append(copy)
    pl.semaphore_signal(tokens.at[0], inc=1, device_id=far_twin, device_id_type=MESH)
    write_ramp(g_ref)
    pl.semaphore_wait(tokens.at[0], 1)

    def spread(block, dh):
        copies = {}
        for far in range(2):
            for dy in range(NY):
                rows = pl.ds(2 * pair_of(y + dy, flip(h, dh)), 2)
                if (far, dy) == (0, 0):
                    cbuf[0, 2 * dh] = block[rows]
                    continue
                copy = pltpu.make_async_remote_copy(
                    src_ref=block.at[rows],
                    dst_ref=cbuf.at[dy, 2 * dh + far],
                    send_sem=c_send.at[dh, dy, far],
                    recv_sem=c_recv.at[dh, dy, far],
                    device_id=near(dy, far, far),
                    device_id_type=MESH,
                )
                copy.start()
                copies[far, dy] = copy
        return copies

    passed = {0: spread(csend, 0)}
    over.wait_recv()
    passed[1] = spread(hbuf, 1)
    for copy in sino:
        copy.wait_recv()
    pl.semaphore_signal(tokens.at[1], inc=1, device_id=sibling, device_id_type=MESH)

    lhs = sbuf[...].reshape(128, 1024)
    for n in range(4):
        total = None
        for m in range(4):
            at = 768 - 256 * m + 256 * n
            term = jnp.dot(
                lhs[:, 256 * m : 256 * (m + 1)], g_ref[:, at : at + 256],
                preferred_element_type=jnp.float32,
            )
            total = term if total is None else total + term
        f_ref[2 * n] = total[:, :128]
        f_ref[2 * n + 1] = total[:, 128:]

    def lay_out(k, carry):
        for a in range(2):
            wide = []
            for low in range(2):
                rows = pl.ds((2 * k + low) * 16 + a, 8, stride=2)
                wide.append([f_ref[n, rows, :] for n in range(8)])
            for n in range(NB):
                block = []
                for parts in wide:
                    if n == 0:
                        block.append(parts[0])
                        continue
                    pair = [parts[n - 1], parts[n] if n < 8 else jnp.zeros_like(parts[0])]
                    turned = [pltpu.roll(part, n, 1) for part in pair]
                    lane = lax.broadcasted_iota(jnp.int32, (8, 128), 1)
                    block.append(jnp.where(lane < n, turned[0], turned[1]))
                v_ref[k, a, 16 * n : 16 * (n + 1), :] = jnp.concatenate(block).astype(jnp.bfloat16)
        return carry

    lax.fori_loop(0, NY, lay_out, 0)

    bins = lax.broadcasted_iota(jnp.int32, (128, 256), 0).astype(jnp.float32).astype(jnp.bfloat16)
    own = z * NC + c
    sent = []
    for dh in range(NH):
        for high in range(2):
            for dy in range(NY):
                if (high, dy) in passed[dh]:
                    passed[dh][high, dy].wait_recv()
            sums = {}
            for dy in range(NY):
                for a in range(2):
                    values = v_ref[dy, a]
                    for row in range(2):
                        for q in range(2):
                            coord = [
                                jnp.broadcast_to(
                                    cbuf[dy, 2 * dh + high, row, a, p : p + 1, :], (8, 128)
                                )
                                for p in (2 * q, 2 * q + 1)
                            ]
                            taps = interpolate(values, jnp.concatenate(coord, axis=1), bins)
                            for low in range(2):
                                at = (row, q, low)
                                sums[at] = sums[at] + taps[low] if at in sums else taps[low]
            if (dh, high) == (0, 0):
                pl.semaphore_wait(tokens.at[1], 1)
            for low in range(2):
                slot = (dh * 2 + high) * 2 + low
                for q in range(2):
                    both = jnp.concatenate([sums[0, q, low], sums[1, q, low]], axis=0)
                    both = (both * jnp.float32(math.pi / 64)).astype(jnp.bfloat16)
                    obuf[slot, :, 256 * q : 256 * (q + 1)] = both
                copy = pltpu.make_async_remote_copy(
                    src_ref=obuf.at[slot],
                    dst_ref=o_ref.at[own],
                    send_sem=o_send.at[slot],
                    recv_sem=o_recv.at[own],
                    device_id=owners[slot],
                    device_id_type=MESH,
                )
                mine = jnp.logical_and(owners[slot][0] == ang, owners[slot][1] == sl)
                keep = pltpu.make_async_copy(obuf.at[slot], o_ref.at[own], own_sem)

                @pl.when(jnp.logical_not(mine))
                def _():
                    copy.start()

                @pl.when(mine)
                def _():
                    keep.start()

                sent.append((copy, keep, mine))

    for copy in [over, *sino, *passed[0].values(), *passed[1].values()]:
        copy.wait_send()

    for copy, keep, mine in sent:

        @pl.when(jnp.logical_not(mine))
        def _():
            copy.wait_send()

        @pl.when(mine)
        def _():
            keep.wait()

    for at, other in enumerate(sources):
        arrival = pltpu.make_async_remote_copy(
            src_ref=obuf.at[0],
            dst_ref=o_ref.at[at],
            send_sem=o_send.at[0],
            recv_sem=o_recv.at[at],
            device_id=other,
            device_id_type=MESH,
        )

        @pl.when(jnp.logical_or(other[0] != ang, other[1] != sl))
        def _():
            arrival.wait_recv()


def shards(sinogram, detector_coord):
    dma = pltpu.SemaphoreType.DMA
    anywhere = pl.BlockSpec(memory_space=pl.ANY)
    partials = pl.pallas_call(
        kernel,
        out_shape=pltpu.VMEM((NZ * NC, 16, 512), jnp.bfloat16),
        in_specs=[anywhere, anywhere],
        out_specs=anywhere,
        scratch_shapes=[
            pltpu.VMEM((2, 8, 512), jnp.int32),
            pltpu.VMEM((8, 2, 4, 128), jnp.int32),
            pltpu.VMEM((8, 2, 4, 128), jnp.int32),
            pltpu.VMEM((2 * NY, 8, 2, 1024), jnp.bfloat16),
            pltpu.VMEM((NY, 4, 2, 2, 4, 128), jnp.int32),
            pltpu.VMEM((256, 1792), jnp.bfloat16),
            pltpu.VMEM((8, 128, 128), jnp.float32),
            pltpu.VMEM((NY, 2, NB * 16, 128), jnp.bfloat16),
            pltpu.VMEM((8, 16, 512), jnp.bfloat16),
            dma((2,)),
            dma((2 * NY,)), dma((2 * NY,)),
            dma(()), dma(()),
            dma((NH, NY, 2)), dma((NH, NY, 2)),
            dma((8,)), dma((8,)),
            dma(()),
            pltpu.SemaphoreType.REGULAR((2,)),
        ],
        compiler_params=pltpu.CompilerParams(collective_id=0, has_side_effects=True),
    )(sinogram, detector_coord)
    return jnp.sum(partials.astype(jnp.float32), axis=0).reshape(2, 8, 512)


def solution(mesh):
    in_specs = (P("sl", "ang", None), P("ang", "sl", None))
    out_specs = P("ang", "sl", None)
    return jax.shard_map(shards, mesh=mesh, in_specs=in_specs, out_specs=out_specs, check_vma=False)
```

```python
import math

import jax
import jax.numpy as jnp
from jax import lax
from jax.experimental import pallas as pl
from jax.experimental.pallas import tpu as pltpu
from jax.sharding import PartitionSpec as P

MESH = pl.DeviceIdType.MESH
NY, NZ, NC, NH, NX = 4, 4, 2, 2, 4
NB, STEP = 9, 127


def flip(bit, by):
    return bit + by - 2 * bit * by


def write_ramp(g_ref):
    depth, width = g_ref.shape

    def chunk(step, carry):
        base = pl.multiple_of(step * 16, 16)
        for lane in range(0, width, 256):
            row = lax.broadcasted_iota(jnp.int32, (16, 256), 0) + base
            column = lax.broadcasted_iota(jnp.int32, (16, 256), 1) + (lane - 768)
            offset = column - row
            real = offset.astype(jnp.float32)
            square = jnp.maximum(real * real, jnp.float32(1.0))
            odd = (offset & 1) != 0
            value = jnp.where(odd, jnp.float32(-1.0 / math.pi**2) / square, jnp.float32(0.0))
            value = jnp.where(offset == 0, jnp.float32(0.25), value)
            g_ref[pl.ds(base, 16), lane : lane + 256] = value.astype(jnp.bfloat16)
        return carry

    lax.fori_loop(0, depth // 16, chunk, 0)


def interpolate(block_values, coord, bins):
    left = coord >> 20
    fraction = (coord & 0xFFFFF).astype(jnp.float32) * jnp.float32(1.0 / 1048576.0)
    block = (left * 8257) >> 20
    within = (left - block * STEP).astype(jnp.float32)

    def rows(value):
        pair = jnp.concatenate([value, value], axis=0).astype(jnp.bfloat16)
        return jnp.concatenate([pair] * 8, axis=0)

    right = jnp.where(bins == rows(within + 1.0), rows(fraction), jnp.zeros((), jnp.bfloat16))
    weights = jnp.where(bins == rows(within), rows(1.0 - fraction), right)
    product = jnp.dot(block_values, weights, preferred_element_type=jnp.float32)
    low, high = product[0:8], product[8:16]
    for n in range(1, NB):
        here = block == n
        low = jnp.where(here, product[16 * n : 16 * n + 8], low)
        high = jnp.where(here, product[16 * n + 8 : 16 * n + 16], high)
    return low, high


def kernel(
    x_ref, c_ref, o_ref,
    cin, csend, hbuf, sbuf, cbuf, g_ref, f_ref, v_ref, obuf,
    in_sem, s_send, s_recv, h_send, h_recv, c_send, c_recv, o_send, o_recv, own_sem, tokens,
):
    load_x = pltpu.make_async_copy(x_ref, sbuf.at[0], in_sem.at[0])
    load_c = pltpu.make_async_copy(c_ref, cin, in_sem.at[1])
    load_x.start()
    load_c.start()
    ang, sl = lax.axis_index("ang"), lax.axis_index("sl")
    y, z, c = ang // 8, (ang // 2) % 4, ang % 2
    h, x = sl // 4, sl % 4
    x_high, x_low = x // 2, x % 2

    def device(yy, zz, cc, hh, xx):
        return (yy * 8 + zz * 2 + cc, hh * 4 + xx)

    def x_at(flip_high, flip_low):
        return flip(x_high, flip_high) * 2 + flip(x_low, flip_low)

    def near(dy, high, low):
        return device((y + dy) % NY, z, c, h, x_at(high, low))

    across = device(y, z, c, flip(h, 1), x)
    sibling = device(y, z, flip(c, 1), h, x)
    far_twin = near(0, 1, 1)
    sharers = [(dy, low) for dy in range(NY) for low in range(2)][1:]
    def pair_of(yy, hh):
        return (yy + 2 * hh) % NY

    owners = []
    for dh in range(NH):
        for far in range(2):
            h_block = flip(h, dh)
            block = h_block * NX + x_at(far, far)
            for low in range(2):
                owners.append((4 * block + pair_of(y, h_block), h * 4 + x_at(0, low)))
    h_row, x_row = ang // 16, (ang // 4) % 4
    source_sl = h * 4 + 2 * x_high + flip(x_row % 2, flip(x_row // 2, x_high))
    source_y = pair_of(ang % 4, h_row)
    sources = [(source_y * 8 + zz * 2 + cc, source_sl) for zz in range(NZ) for cc in range(NC)]

    barrier = pltpu.get_barrier_semaphore()
    group = [across, far_twin, sibling] + [near(dy, 0, low) for dy, low in sharers]
    group += [device(y, (z + dz) % NZ, c, h, x) for dz in range(1, NZ)]
    for other in group:
        pl.semaphore_signal(barrier, inc=1, device_id=other, device_id_type=MESH)
    load_c.wait()
    for a in range(2):
        for p in range(4):
            csend[:, a, p, :] = cin[a, :, 128 * p : 128 * (p + 1)]
    load_x.wait()
    pl.semaphore_wait(barrier, len(group))

    over = pltpu.make_async_remote_copy(
        src_ref=csend, dst_ref=hbuf, send_sem=h_send, recv_sem=h_recv,
        device_id=across, device_id_type=MESH,
    )
    over.start()

    sino = []
    for dy, low in sharers:
        k = dy * 2 + low
        copy = pltpu.make_async_remote_copy(
            src_ref=sbuf.at[0],
            dst_ref=sbuf.at[k],
            send_sem=s_send.at[k],
            recv_sem=s_recv.at[k],
            device_id=near(dy, 0, low),
            device_id_type=MESH,
        )
        copy.start()
        sino.append(copy)
    pl.semaphore_signal(tokens.at[0], inc=1, device_id=far_twin, device_id_type=MESH)
    write_ramp(g_ref)
    pl.semaphore_wait(tokens.at[0], 1)

    def spread(block, dh):
        copies = {}
        for far in range(2):
            for dy in range(NY):
                rows = pl.ds(2 * pair_of(y + dy, flip(h, dh)), 2)
                if (far, dy) == (0, 0):
                    cbuf[0, 2 * dh] = block[rows]
                    continue
                copy = pltpu.make_async_remote_copy(
                    src_ref=block.at[rows],
                    dst_ref=cbuf.at[dy, 2 * dh + far],
                    send_sem=c_send.at[dh, dy, far],
                    recv_sem=c_recv.at[dh, dy, far],
                    device_id=near(dy, far, far),
                    device_id_type=MESH,
                )
                copy.start()
                copies[far, dy] = copy
        return copies

    passed = {0: spread(csend, 0)}
    over.wait_recv()
    passed[1] = spread(hbuf, 1)
    for copy in sino:
        copy.wait_recv()
    pl.semaphore_signal(tokens.at[1], inc=1, device_id=sibling, device_id_type=MESH)

    lhs = sbuf[...].reshape(128, 1024)
    for n in range(4):
        total = None
        for m in range(4):
            at = 768 - 256 * m + 256 * n
            term = jnp.dot(
                lhs[:, 256 * m : 256 * (m + 1)], g_ref[:, at : at + 256],
                preferred_element_type=jnp.float32,
            )
            total = term if total is None else total + term
        f_ref[2 * n] = total[:, :128]
        f_ref[2 * n + 1] = total[:, 128:]

    def lay_out(k, carry):
        for a in range(2):
            wide = []
            for low in range(2):
                rows = pl.ds((2 * k + low) * 16 + a, 8, stride=2)
                wide.append([f_ref[n, rows, :] for n in range(8)])
            for n in range(NB):
                block = []
                for parts in wide:
                    if n == 0:
                        block.append(parts[0])
                        continue
                    pair = [parts[n - 1], parts[n] if n < 8 else jnp.zeros_like(parts[0])]
                    turned = [pltpu.roll(part, n, 1) for part in pair]
                    lane = lax.broadcasted_iota(jnp.int32, (8, 128), 1)
                    block.append(jnp.where(lane < n, turned[0], turned[1]))
                v_ref[k, a, 16 * n : 16 * (n + 1), :] = jnp.concatenate(block).astype(jnp.bfloat16)
        return carry

    lax.fori_loop(0, NY, lay_out, 0)

    bins = lax.broadcasted_iota(jnp.int32, (128, 256), 0).astype(jnp.float32).astype(jnp.bfloat16)
    own = z * NC + c
    sent = []
    for dh in range(NH):
        for high in range(2):
            for dy in range(NY):
                if (high, dy) in passed[dh]:
                    passed[dh][high, dy].wait_recv()
            sums = {}
            for dy in range(NY):
                for a in range(2):
                    values = v_ref[dy, a]
                    for row in range(2):
                        for q in range(2):
                            coord = [
                                jnp.broadcast_to(
                                    cbuf[dy, 2 * dh + high, row, a, p : p + 1, :], (8, 128)
                                )
                                for p in (2 * q, 2 * q + 1)
                            ]
                            taps = interpolate(values, jnp.concatenate(coord, axis=1), bins)
                            for low in range(2):
                                at = (row, q, low)
                                sums[at] = sums[at] + taps[low] if at in sums else taps[low]
            if (dh, high) == (0, 0):
                pl.semaphore_wait(tokens.at[1], 1)
            for low in (1, 0):
                slot = (dh * 2 + high) * 2 + low
                for q in range(2):
                    both = jnp.concatenate([sums[0, q, low], sums[1, q, low]], axis=0)
                    both = (both * jnp.float32(math.pi / 64)).astype(jnp.bfloat16)
                    obuf[slot, :, 256 * q : 256 * (q + 1)] = both
                copy = pltpu.make_async_remote_copy(
                    src_ref=obuf.at[slot],
                    dst_ref=o_ref.at[own],
                    send_sem=o_send.at[slot],
                    recv_sem=o_recv.at[own],
                    device_id=owners[slot],
                    device_id_type=MESH,
                )
                mine = jnp.logical_and(owners[slot][0] == ang, owners[slot][1] == sl)
                keep = pltpu.make_async_copy(obuf.at[slot], o_ref.at[own], own_sem)

                @pl.when(jnp.logical_not(mine))
                def _():
                    copy.start()

                @pl.when(mine)
                def _():
                    keep.start()

                sent.append((copy, keep, mine))

    for copy in [over, *sino, *passed[0].values(), *passed[1].values()]:
        copy.wait_send()

    for copy, keep, mine in sent:

        @pl.when(jnp.logical_not(mine))
        def _():
            copy.wait_send()

        @pl.when(mine)
        def _():
            keep.wait()

    for at, other in enumerate(sources):
        arrival = pltpu.make_async_remote_copy(
            src_ref=obuf.at[0],
            dst_ref=o_ref.at[at],
            send_sem=o_send.at[0],
            recv_sem=o_recv.at[at],
            device_id=other,
            device_id_type=MESH,
        )

        @pl.when(jnp.logical_or(other[0] != ang, other[1] != sl))
        def _():
            arrival.wait_recv()


def shards(sinogram, detector_coord):
    dma = pltpu.SemaphoreType.DMA
    anywhere = pl.BlockSpec(memory_space=pl.ANY)
    partials = pl.pallas_call(
        kernel,
        out_shape=pltpu.VMEM((NZ * NC, 16, 512), jnp.bfloat16),
        in_specs=[anywhere, anywhere],
        out_specs=anywhere,
        scratch_shapes=[
            pltpu.VMEM((2, 8, 512), jnp.int32),
            pltpu.VMEM((8, 2, 4, 128), jnp.int32),
            pltpu.VMEM((8, 2, 4, 128), jnp.int32),
            pltpu.VMEM((2 * NY, 8, 2, 1024), jnp.bfloat16),
            pltpu.VMEM((NY, 4, 2, 2, 4, 128), jnp.int32),
            pltpu.VMEM((256, 1792), jnp.bfloat16),
            pltpu.VMEM((8, 128, 128), jnp.float32),
            pltpu.VMEM((NY, 2, NB * 16, 128), jnp.bfloat16),
            pltpu.VMEM((8, 16, 512), jnp.bfloat16),
            dma((2,)),
            dma((2 * NY,)), dma((2 * NY,)),
            dma(()), dma(()),
            dma((NH, NY, 2)), dma((NH, NY, 2)),
            dma((8,)), dma((8,)),
            dma(()),
            pltpu.SemaphoreType.REGULAR((2,)),
        ],
        compiler_params=pltpu.CompilerParams(collective_id=0, has_side_effects=True),
    )(sinogram, detector_coord)
    return jnp.sum(partials.astype(jnp.float32), axis=0).reshape(2, 8, 512)


def solution(mesh):
    in_specs = (P("sl", "ang", None), P("ang", "sl", None))
    out_specs = P("ang", "sl", None)
    return jax.shard_map(shards, mesh=mesh, in_specs=in_specs, out_specs=out_specs, check_vma=False)
```

```python
import math

import jax
import jax.numpy as jnp
from jax import lax
from jax.experimental import pallas as pl
from jax.experimental.pallas import tpu as pltpu
from jax.sharding import PartitionSpec as P

MESH = pl.DeviceIdType.MESH
NY, NZ, NC, NH, NX = 4, 4, 2, 2, 4
NB, STEP = 9, 127


def flip(bit, by):
    return bit + by - 2 * bit * by


def write_ramp(g_ref):
    depth, width = g_ref.shape

    def chunk(step, carry):
        base = pl.multiple_of(step * 16, 16)
        for lane in range(0, width, 256):
            row = lax.broadcasted_iota(jnp.int32, (16, 256), 0) + base
            column = lax.broadcasted_iota(jnp.int32, (16, 256), 1) + (lane - 768)
            offset = column - row
            real = offset.astype(jnp.float32)
            square = jnp.maximum(real * real, jnp.float32(1.0))
            odd = (offset & 1) != 0
            value = jnp.where(odd, jnp.float32(-1.0 / math.pi**2) / square, jnp.float32(0.0))
            value = jnp.where(offset == 0, jnp.float32(0.25), value)
            g_ref[pl.ds(base, 16), lane : lane + 256] = value.astype(jnp.bfloat16)
        return carry

    lax.fori_loop(0, depth // 16, chunk, 0)


def interpolate(block_values, coord, bins):
    left = coord >> 20
    fraction = (coord & 0xFFFFF).astype(jnp.float32) * jnp.float32(1.0 / 1048576.0)
    block = (left * 8257) >> 20
    within = (left - block * STEP).astype(jnp.float32)

    def rows(value):
        pair = jnp.concatenate([value, value], axis=0).astype(jnp.bfloat16)
        return jnp.concatenate([pair] * 8, axis=0)

    right = jnp.where(bins == rows(within + 1.0), rows(fraction), jnp.zeros((), jnp.bfloat16))
    weights = jnp.where(bins == rows(within), rows(1.0 - fraction), right)
    product = jnp.dot(block_values, weights, preferred_element_type=jnp.float32)
    low, high = product[0:8], product[8:16]
    for n in range(1, NB):
        here = block == n
        low = jnp.where(here, product[16 * n : 16 * n + 8], low)
        high = jnp.where(here, product[16 * n + 8 : 16 * n + 16], high)
    return low, high


def kernel(
    x_ref, c_ref, o_ref,
    cin, csend, hbuf, sbuf, cbuf, g_ref, f_ref, v_ref, obuf,
    in_sem, s_send, s_recv, h_send, h_recv, c_send, c_recv, o_send, o_recv, own_sem, tokens,
):
    load_x = pltpu.make_async_copy(x_ref, sbuf.at[0], in_sem.at[0])
    load_c = pltpu.make_async_copy(c_ref, cin, in_sem.at[1])
    load_x.start()
    load_c.start()
    ang, sl = lax.axis_index("ang"), lax.axis_index("sl")
    y, z, c = ang // 8, (ang // 2) % 4, ang % 2
    h, x = sl // 4, sl % 4
    x_high, x_low = x // 2, x % 2

    def device(yy, zz, cc, hh, xx):
        return (yy * 8 + zz * 2 + cc, hh * 4 + xx)

    def x_at(flip_high, flip_low):
        return flip(x_high, flip_high) * 2 + flip(x_low, flip_low)

    def near(dy, high, low):
        return device((y + dy) % NY, z, c, h, x_at(high, low))

    across = device(y, z, c, flip(h, 1), x)
    sibling = device(y, z, flip(c, 1), h, x)
    far_twin = near(0, 1, 1)
    twin = near(0, 0, 1)
    sharers = [(0, 1), (1, 0), (1, 1), (3, 0), (3, 1), (2, 0), (2, 1)]
    def pair_of(yy, hh):
        return (yy + 2 * hh) % NY

    owners = []
    for dh in range(NH):
        for far in range(2):
            h_block = flip(h, dh)
            block = h_block * NX + x_at(far, far)
            for low in range(2):
                owners.append((4 * block + pair_of(y, h_block), h * 4 + x_at(0, low)))
    h_row, x_row = ang // 16, (ang // 4) % 4
    source_sl = h * 4 + 2 * x_high + flip(x_row % 2, flip(x_row // 2, x_high))
    source_y = pair_of(ang % 4, h_row)
    sources = [(source_y * 8 + zz * 2 + cc, source_sl) for zz in range(NZ) for cc in range(NC)]

    barrier = pltpu.get_barrier_semaphore()
    group = [across, far_twin, sibling] + [near(dy, 0, low) for dy, low in sharers[:-1]]
    group += [device(y, (z + dz) % NZ, c, h, x) for dz in range(1, NZ)]
    for other in group:
        pl.semaphore_signal(barrier, inc=1, device_id=other, device_id_type=MESH)
    load_c.wait()
    for a in range(2):
        for p in range(4):
            csend[:, a, p, :] = cin[a, :, 128 * p : 128 * (p + 1)]
    load_x.wait()
    pl.semaphore_wait(barrier, len(group))

    over = pltpu.make_async_remote_copy(
        src_ref=csend, dst_ref=hbuf, send_sem=h_send, recv_sem=h_recv,
        device_id=across, device_id_type=MESH,
    )
    over.start()

    sino = []
    pl.semaphore_signal(tokens.at[0], inc=1, device_id=far_twin, device_id_type=MESH)
    pl.semaphore_signal(tokens.at[2], inc=1, device_id=twin, device_id_type=MESH)
    for dy, low in sharers:
        if (dy, low) == sharers[-1]:
            pl.semaphore_wait(tokens.at[2], 1)
        k = dy * 2 + low
        copy = pltpu.make_async_remote_copy(
            src_ref=sbuf.at[0],
            dst_ref=sbuf.at[k],
            send_sem=s_send.at[k],
            recv_sem=s_recv.at[k],
            device_id=near(dy, 0, low),
            device_id_type=MESH,
        )
        copy.start()
        sino.append(copy)
    write_ramp(g_ref)
    pl.semaphore_wait(tokens.at[0], 1)

    def spread(block, dh):
        copies = {}
        for far in range(2):
            for dy in range(NY):
                rows = pl.ds(2 * pair_of(y + dy, flip(h, dh)), 2)
                if (far, dy) == (0, 0):
                    cbuf[0, 2 * dh] = block[rows]
                    continue
                copy = pltpu.make_async_remote_copy(
                    src_ref=block.at[rows],
                    dst_ref=cbuf.at[dy, 2 * dh + far],
                    send_sem=c_send.at[dh, dy, far],
                    recv_sem=c_recv.at[dh, dy, far],
                    device_id=near(dy, far, far),
                    device_id_type=MESH,
                )
                copy.start()
                copies[far, dy] = copy
        return copies

    passed = {0: spread(csend, 0)}
    over.wait_recv()
    passed[1] = spread(hbuf, 1)
    for copy in sino:
        copy.wait_recv()
    pl.semaphore_signal(tokens.at[1], inc=1, device_id=sibling, device_id_type=MESH)

    lhs = sbuf[...].reshape(128, 1024)
    for n in range(4):
        total = None
        for m in range(4):
            at = 768 - 256 * m + 256 * n
            term = jnp.dot(
                lhs[:, 256 * m : 256 * (m + 1)], g_ref[:, at : at + 256],
                preferred_element_type=jnp.float32,
            )
            total = term if total is None else total + term
        f_ref[2 * n] = total[:, :128]
        f_ref[2 * n + 1] = total[:, 128:]

    def lay_out(k, carry):
        for a in range(2):
            wide = []
            for low in range(2):
                rows = pl.ds((2 * k + low) * 16 + a, 8, stride=2)
                wide.append([f_ref[n, rows, :] for n in range(8)])
            for n in range(NB):
                block = []
                for parts in wide:
                    if n == 0:
                        block.append(parts[0])
                        continue
                    pair = [parts[n - 1], parts[n] if n < 8 else jnp.zeros_like(parts[0])]
                    turned = [pltpu.roll(part, n, 1) for part in pair]
                    lane = lax.broadcasted_iota(jnp.int32, (8, 128), 1)
                    block.append(jnp.where(lane < n, turned[0], turned[1]))
                v_ref[k, a, 16 * n : 16 * (n + 1), :] = jnp.concatenate(block).astype(jnp.bfloat16)
        return carry

    lax.fori_loop(0, NY, lay_out, 0)

    bins = lax.broadcasted_iota(jnp.int32, (128, 256), 0).astype(jnp.float32).astype(jnp.bfloat16)
    own = z * NC + c
    sent = []
    for dh in range(NH):
        for high in range(2):
            for dy in range(NY):
                if (high, dy) in passed[dh]:
                    passed[dh][high, dy].wait_recv()
            sums = {}
            for dy in range(NY):
                for a in range(2):
                    values = v_ref[dy, a]
                    for row in range(2):
                        for q in range(2):
                            coord = [
                                jnp.broadcast_to(
                                    cbuf[dy, 2 * dh + high, row, a, p : p + 1, :], (8, 128)
                                )
                                for p in (2 * q, 2 * q + 1)
                            ]
                            taps = interpolate(values, jnp.concatenate(coord, axis=1), bins)
                            for low in range(2):
                                at = (row, q, low)
                                sums[at] = sums[at] + taps[low] if at in sums else taps[low]
            if (dh, high) == (0, 0):
                pl.semaphore_wait(tokens.at[1], 1)
            for low in (1, 0):
                slot = (dh * 2 + high) * 2 + low
                for q in range(2):
                    both = jnp.concatenate([sums[0, q, low], sums[1, q, low]], axis=0)
                    both = (both * jnp.float32(math.pi / 64)).astype(jnp.bfloat16)
                    obuf[slot, :, 256 * q : 256 * (q + 1)] = both
                copy = pltpu.make_async_remote_copy(
                    src_ref=obuf.at[slot],
                    dst_ref=o_ref.at[own],
                    send_sem=o_send.at[slot],
                    recv_sem=o_recv.at[own],
                    device_id=owners[slot],
                    device_id_type=MESH,
                )
                mine = jnp.logical_and(owners[slot][0] == ang, owners[slot][1] == sl)
                keep = pltpu.make_async_copy(obuf.at[slot], o_ref.at[own], own_sem)

                @pl.when(jnp.logical_not(mine))
                def _():
                    copy.start()

                @pl.when(mine)
                def _():
                    keep.start()

                sent.append((copy, keep, mine))

    for copy in [over, *sino, *passed[0].values(), *passed[1].values()]:
        copy.wait_send()

    for copy, keep, mine in sent:

        @pl.when(jnp.logical_not(mine))
        def _():
            copy.wait_send()

        @pl.when(mine)
        def _():
            keep.wait()

    for at, other in enumerate(sources):
        arrival = pltpu.make_async_remote_copy(
            src_ref=obuf.at[0],
            dst_ref=o_ref.at[at],
            send_sem=o_send.at[0],
            recv_sem=o_recv.at[at],
            device_id=other,
            device_id_type=MESH,
        )

        @pl.when(jnp.logical_or(other[0] != ang, other[1] != sl))
        def _():
            arrival.wait_recv()


def shards(sinogram, detector_coord):
    dma = pltpu.SemaphoreType.DMA
    anywhere = pl.BlockSpec(memory_space=pl.ANY)
    partials = pl.pallas_call(
        kernel,
        out_shape=pltpu.VMEM((NZ * NC, 16, 512), jnp.bfloat16),
        in_specs=[anywhere, anywhere],
        out_specs=anywhere,
        scratch_shapes=[
            pltpu.VMEM((2, 8, 512), jnp.int32),
            pltpu.VMEM((8, 2, 4, 128), jnp.int32),
            pltpu.VMEM((8, 2, 4, 128), jnp.int32),
            pltpu.VMEM((2 * NY, 8, 2, 1024), jnp.bfloat16),
            pltpu.VMEM((NY, 4, 2, 2, 4, 128), jnp.int32),
            pltpu.VMEM((256, 1792), jnp.bfloat16),
            pltpu.VMEM((8, 128, 128), jnp.float32),
            pltpu.VMEM((NY, 2, NB * 16, 128), jnp.bfloat16),
            pltpu.VMEM((8, 16, 512), jnp.bfloat16),
            dma((2,)),
            dma((2 * NY,)), dma((2 * NY,)),
            dma(()), dma(()),
            dma((NH, NY, 2)), dma((NH, NY, 2)),
            dma((8,)), dma((8,)),
            dma(()),
            pltpu.SemaphoreType.REGULAR((3,)),
        ],
        compiler_params=pltpu.CompilerParams(collective_id=0, has_side_effects=True),
    )(sinogram, detector_coord)
    return jnp.sum(partials.astype(jnp.float32), axis=0).reshape(2, 8, 512)


def solution(mesh):
    in_specs = (P("sl", "ang", None), P("ang", "sl", None))
    out_specs = P("ang", "sl", None)
    return jax.shard_map(shards, mesh=mesh, in_specs=in_specs, out_specs=out_specs, check_vma=False)
```
